32 devices in a mesh: gx: 2 (over core), gy: 4 (over y, x), gz: 4 (over z).
Axes of the slice: x: 2, y: 2, z: 4, core: 2. Of those that a mesh axis runs over, the one named last changes fastest.
Arguments:
- queries: bfloat16 [128, 32, 128], P(None, 'gy'), may hold values from -6 to 6
- passages: bfloat16 [1024, 256, 128], P('gx', 'gz'), may hold values from -0.5 to 0.5
- passage_len: int32 [1024], P('gx'), may hold values from 32 to 256
- query_len: int32 [128], replicated, may hold values from 8 to 32
Outputs:
- log_probs: float32 [128, 1024], P(None, ('gx', 'gz'))
The draws below stay inside these ranges and needn't reach their ends.
All inputs are finite; a program needn't handle non-finite values.
Results may differ from the reference program's by a relative error of at most 0.0003.
Values sent between devices are 32-bit elements; how exact they have to be, the bound alone decides.
A program may use at most 64 MiB of HBM per device.

```python
import math
import jax
import jax.numpy as jnp
from jax import lax

DIM = 128
NQ = 128
LQ = 32
LP = 256
NP = 1024


def draw_queries(key, part):
    noise_key = jax.random.fold_in(key, 11)
    values = jnp.clip(jax.random.normal(noise_key, (NQ, LQ, DIM), jnp.float32), -6.0, 6.0)
    return values.astype(jnp.bfloat16)


def draw_passages(key, part):
    noise_key = jax.random.fold_in(key, 21)
    values = jax.random.normal(noise_key, (NP, LP, DIM), jnp.float32) * DIM ** (-0.5)
    values = jnp.clip(values, -0.5, 0.5)
    return values.astype(jnp.bfloat16)


def set_ends(entries, stream_key, smallest, high):
    spot = [jax.random.randint(jax.random.fold_in(stream_key, axis), (), 0, length) for axis, length in enumerate(entries.shape)]
    main_axis = entries.shape.index(max(entries.shape))
    beside = spot[:main_axis] + [(spot[main_axis] + 1) % entries.shape[main_axis]] + spot[main_axis + 1:]
    return entries.at[tuple(spot)].set(smallest).at[tuple(beside)].set(high)


def setup_inputs(seed: int = 0) -> dict:
    arg_keys = jax.random.split(jax.random.key(seed), 5)
    queries = draw_queries(jax.random.fold_in(arg_keys[4], 71), 0)
    passages = draw_passages(jax.random.fold_in(arg_keys[4], 71), 0)
    passage_len = set_ends(jax.random.randint(arg_keys[2], (NP,), LP // 8, LP + 1), jax.random.fold_in(arg_keys[2], 1), LP // 8, LP).astype(jnp.int32)
    query_len = set_ends(jax.random.randint(arg_keys[3], (NQ,), max(1, LQ // 4), LQ + 1), jax.random.fold_in(arg_keys[3], 1), max(1, LQ // 4), LQ).astype(jnp.int32)
    return dict(queries=queries, passages=passages, passage_len=passage_len, query_len=query_len)


masked_low = -1.0e30


def reference(queries, passages, passage_len, query_len):
    flat_queries = queries.reshape(NQ * LQ, DIM)
    per_block = math.gcd(NP, 32)
    num_blocks = NP // per_block
    tile_stack = passages.reshape(num_blocks, per_block * LP, DIM)
    length_stack = passage_len.reshape(num_blocks, per_block)
    query_used = jnp.arange(LQ, dtype=jnp.int32)[None, :] < query_len[:, None]
    token_ids = jnp.arange(LP, dtype=jnp.int32)

    def block_scores(packed):
        passage_tile, tile_len = packed
        scores = jnp.dot(flat_queries, passage_tile.T, preferred_element_type=jnp.float32)
        scores = scores.reshape(NQ * LQ, per_block, LP)
        usable = token_ids[None, :] < tile_len[:, None]
        scores = jnp.where(usable[None], scores, masked_low)
        maxima = jnp.max(scores, axis=2).reshape(NQ, LQ, per_block)
        return jnp.sum(jnp.where(query_used[:, :, None], maxima, 0.0), axis=1)

    pieces = lax.map(block_scores, (tile_stack, length_stack))
    maxsim = jnp.transpose(pieces, (1, 0, 2)).reshape(NQ, NP)
    highest = jnp.max(maxsim, axis=1, keepdims=True)
    summed = jnp.sum(jnp.exp(maxsim - highest), axis=1, keepdims=True)
    return maxsim - (highest + jnp.log(summed))
```

```python
import functools

import jax
import jax.numpy as jnp
from jax import lax
from jax.experimental import pallas as pl
from jax.experimental.pallas import tpu as pltpu
from jax.sharding import PartitionSpec as P

masked_low = -1e30
MESH = pl.DeviceIdType.MESH
UP_LAGS = (3, 3)
DOWN_LAGS = (4, 3)
PEER_LAG = 3
TAIL = 2
PER_CHUNK = 16


def kernel(
    sizes,
    queries_in,
    lengths_in,
    query_len_in,
    passages,
    out,
    queries,
    lengths,
    query_len,
    x,
    masked_x,
    wide_queries,
    query_columns,
    limits,
    own_low,
    own_high,
    got_low,
    got_high,
    partials,
    forward,
    total,
    stats,
    far_tail,
    out_tile,
    small_sem,
    load_sem,
    z_send,
    out_sem,
    low_recv,
    high_recv,
    peer_send,
    peer_recv,
    forward_send,
    forward_recv,
    stat_send,
    stat_recv,
    far_send,
    far_recv,
):
    nx, ny, nz = sizes
    gx, gy, gz = (lax.axis_index(name) for name in ("gx", "gy", "gz"))
    passage_count, token_count, width = x.shape
    query_count, query_rows, _ = queries.shape
    slots, per_chunk, row_count = own_low.shape
    chunks = slots - 1
    half_blocks = nz // 2
    per_block = chunks // half_blocks
    block_rows = passage_count // nz

    def low_start(c):
        return (half_blocks - 1 - c // per_block) * block_rows + (c % per_block) * per_chunk

    def high_start(c):
        return half_blocks * block_rows + c * per_chunk

    barrier = pltpu.get_barrier_semaphore()
    for axis, place, count in (("gx", gx, nx), ("gy", gy, ny)):
        for turn in range(1, count):
            pl.semaphore_signal(
                barrier,
                inc=1,
                device_id={axis: lax.rem(place + turn, count)},
                device_id_type=MESH,
            )
    for has_neighbour, neighbour in ((gz > 0, gz - 1), (gz < nz - 1, gz + 1)):
        @pl.when(has_neighbour)
        def _():
            pl.semaphore_signal(
                barrier, inc=1, device_id={"gz": neighbour}, device_id_type=MESH
            )

    at_end = (gz == 0) | (gz == nz - 1)

    small = [
        pltpu.make_async_copy(source, target, small_sem.at[index])
        for index, (source, target) in enumerate(
            ((queries_in, queries), (lengths_in, lengths), (query_len_in, query_len))
        )
    ]
    for copy in small:
        copy.start()

    def load(start, index):
        rows = pl.ds(start, per_chunk)
        return pltpu.make_async_copy(passages.at[rows], x.at[rows], load_sem.at[index])

    def start_loads(c, carry):
        load(low_start(c), c).start()
        load(high_start(c), chunks + c).start()
        return carry

    lax.fori_loop(0, chunks, start_loads, 0)

    for copy in small:
        copy.wait()

    wide_queries[...] = queries[...].astype(jnp.float32).reshape(row_count, width)
    for i in range(query_rows):
        tile = wide_queries[pl.ds(i, query_count, stride=query_rows), :]
        query_columns[:, i * query_count : (i + 1) * query_count] = tile.T.astype(jnp.bfloat16)

    first_token = (gz * token_count).astype(jnp.float32)
    for b in range(passage_count // 128):
        row = lengths[b : b + 1, :].astype(jnp.float32) - first_token
        limits[b * 128 : (b + 1) * 128, :] = jnp.broadcast_to(row, (128, 128)).T

    token_ids = lax.broadcasted_iota(jnp.int32, (token_count, width), 0).astype(jnp.float32)
    tile_columns = 256

    def compute(c):
        starts = (low_start(c), high_start(c))
        limit = []
        for half, start in enumerate(starts):
            for p in range(per_chunk):
                tokens = x[start + p].astype(jnp.float32)
                usable = token_ids < limits[pl.ds(start + p, 1), :]
                tokens = jnp.where(usable, tokens, tokens[0:1, :])
                row = (half * per_chunk + p) * token_count
                masked_x[row : row + token_count, :] = tokens.astype(jnp.bfloat16)
            limit.append(limits[pl.ds(start, per_chunk), :])
        limit = jnp.concatenate(limit, axis=0)
        any_used = jnp.concatenate([limit] * (tile_columns // 128), axis=1) > 0.0
        for t in range(row_count // tile_columns):
            columns = slice(t * tile_columns, (t + 1) * tile_columns)
            scores = jnp.dot(
                masked_x[...], query_columns[:, columns], preferred_element_type=jnp.float32
            )
            best = jnp.max(scores.reshape(2 * per_chunk, token_count, tile_columns), axis=1)
            best = jnp.where(any_used, best, masked_low)
            own_low[c, :, columns] = best[:per_chunk]
            own_high[c, :, columns] = best[per_chunk:]

    class Flow:
        def __init__(self, own, got, recv, index, hops, lags, target):
            self.own, self.got, self.recv, self.index = own, got, recv, index
            self.target = target
            self.is_first, self.is_last = hops == 0, hops == nz - 1
            self.is_inner = (hops > 0) & (hops < nz - 1)
            self.lag = lags[0] + lags[1] * (hops - 1)

        def copy(self, source, c):
            return pltpu.make_async_remote_copy(
                src_ref=source.at[c],
                dst_ref=self.got.at[c],
                send_sem=z_send.at[self.index],
                recv_sem=self.recv.at[c],
                device_id={"gz": self.target},
                device_id_type=MESH,
            )

        def merge(self, c):
            self.got[c] = jnp.maximum(self.got[c], self.own[c])

    first, last = gz == 0, gz == nz - 1
    below, above = lax.rem(gz + nz - 1, nz), lax.rem(gz + 1, nz)
    low = Flow(own_low, got_low, low_recv, 0, nz - 1 - gz, DOWN_LAGS, below)
    high = Flow(own_high, got_high, high_recv, 1, gz, UP_LAGS, above)
    flows = (low, high)

    def peer_copy(turn, slot, block, where):
        return pltpu.make_async_remote_copy(
            src_ref=partials.at[(slot, *where)],
            dst_ref=partials.at[(slot, *where)],
            send_sem=peer_send.at[turn],
            recv_sem=peer_recv.at[slot, block],
            device_id={"gy": lax.rem(gy + turn, ny)},
            device_id_type=MESH,
        )

    def finalise(merged, c):
        counted = query_len[...] - gy * query_rows
        so_far = jnp.zeros((per_chunk, query_count), jnp.float32)
        for i in range(query_rows):
            values = merged[c, :, i * query_count : (i + 1) * query_count]
            so_far = so_far + jnp.where(counted > i, values, 0.0)
        partials[gy, c] = so_far
        for turn in range(1, ny):
            peer_copy(turn, gy, piece_of(c), (c,)).start()

    def piece_of(c):
        return c // per_block + jnp.where(c >= chunks - TAIL, 1, 0)

    def piece_total(piece):
        start = piece * per_block if piece < half_blocks else chunks - TAIL
        count = TAIL if piece == half_blocks else per_block - TAIL * (piece == half_blocks - 1)
        where = pl.ds(start, count)
        for turn in range(1, ny):
            slot = lax.rem(gy + turn, ny)
            peer_copy(turn, slot, piece, (where,)).wait_recv()
        summed = partials[0, where]
        for slot in range(1, ny):
            summed = summed + partials[slot, where]
        return summed.reshape(count * per_chunk, query_count)

    def far_copy(turn, slot):
        tail = pl.ds(chunks - TAIL, TAIL)
        return pltpu.make_async_remote_copy(
            src_ref=partials.at[slot, tail],
            dst_ref=far_tail.at[slot],
            send_sem=far_send.at[turn],
            recv_sem=far_recv.at[slot],
            device_id={"gy": lax.rem(gy + turn, ny), "gz": 0},
            device_id_type=MESH,
        )

    def forward_copy(block):
        target = jnp.where(gz == 0, half_blocks - 1 - block, half_blocks + block)
        return pltpu.make_async_remote_copy(
            src_ref=forward.at[block],
            dst_ref=total,
            send_sem=forward_send.at[block],
            recv_sem=forward_recv,
            device_id={"gz": target},
            device_id_type=MESH,
        )

    def receive(flow, c):
        flow.copy(flow.got, c).wait_recv()
        flow.merge(c)
        flow.copy(flow.got, c).start()

    def ready(s):
        load(low_start(s), s).wait()
        load(high_start(s), chunks + s).wait()
        compute(s)

    def send(flow, c):
        @pl.when(flow.is_first)
        def _():
            flow.copy(flow.own, c).start()

    def pass_on(s):
        for flow in flows:
            c = s - flow.lag

            @pl.when(flow.is_inner & (c >= 0) & (c < chunks))
            def _():
                receive(flow, c)

    def head(s, carry):
        ready(s)
        return carry

    def head_send(c, carry):
        for flow in flows:
            send(flow, c)
        return carry

    def step(s, carry):
        pass_on(s)
        ready(s)
        for flow in flows:
            send(flow, s)
        return carry

    def drain(s, carry):
        pass_on(s)
        return carry

    last_lag = max(lags[0] + lags[1] * (nz - 3) for lags in (UP_LAGS, DOWN_LAGS))
    head_steps = 1
    lax.fori_loop(0, head_steps, head, 0)
    pl.semaphore_wait(barrier, nx + ny - 2 + jnp.where(at_end, 1, 2))
    lax.fori_loop(0, head_steps, head_send, 0)
    lax.fori_loop(head_steps, chunks, step, 0)

    @pl.when(jnp.logical_not(at_end))
    def _():
        lax.fori_loop(chunks, chunks + last_lag, drain, 0)

    for flow in flows:
        @pl.when(flow.is_last)
        def _():
            def collect(c, carry):
                flow.copy(flow.got, c).wait_recv()
                flow.merge(c)
                finalise(flow.got, c)
                for block in range(half_blocks - 1):
                    @pl.when(c == (block + 1) * per_block - 1 + PEER_LAG)
                    def _():
                        forward[block] = piece_total(block)
                        forward_copy(block).start()
                return carry

            lax.fori_loop(0, chunks, collect, 0)

    main_rows = block_rows - TAIL * per_chunk
    row_ids = lax.broadcasted_iota(jnp.int32, stats.shape[1:], 0)

    def stat_copy(axis, base, place, count, slot, turn):
        return pltpu.make_async_remote_copy(
            src_ref=stats.at[base + slot],
            dst_ref=stats.at[base + slot],
            send_sem=stat_send.at[base + turn],
            recv_sem=stat_recv.at[base + slot],
            device_id={axis: lax.rem(place + turn, count)},
            device_id_type=MESH,
        )

    def share(axis, base, place, count, slot):
        for turn in range(1, count):
            stat_copy(axis, base, place, count, slot, turn).start()

    def pair(top, summed):
        return jnp.where(row_ids == 0, top, summed)

    def joined(pairs):
        highest = functools.reduce(jnp.maximum, [top for top, _ in pairs])
        shares = [summed * jnp.exp(top - highest) for top, summed in pairs]
        return highest, functools.reduce(jnp.add, shares)

    def summary(blocks):
        tops = [jnp.max(block, axis=0, keepdims=True) for block in blocks]
        top = functools.reduce(jnp.maximum, tops)
        sums = [jnp.sum(jnp.exp(block - top), axis=0, keepdims=True) for block in blocks]
        return top, functools.reduce(jnp.add, sums)

    def read(slot):
        return stats[slot, 0:1, :], stats[slot, 1:2, :]

    def main_summary():
        total[pl.ds(0, main_rows), :] = piece_total(half_blocks - 1)
        blocks = [forward[block] for block in range(half_blocks - 1)]
        return summary(blocks + [total[pl.ds(0, main_rows), :]])

    far_stat = stat_copy("gz", nx, gz, nz, 0, 1)
    final_stat = stat_copy("gz", nx, gz, nz, 1, 1)

    @pl.when(last)
    def _():
        for turn in range(ny):
            far_copy(turn, gy).start()
        stats[nx] = pair(*main_summary())
        far_stat.start()
        total[pl.ds(main_rows, TAIL * per_chunk), :] = piece_total(half_blocks)

    @pl.when(jnp.logical_not(at_end))
    def _():
        forward_copy(0).wait_recv()

    @pl.when(first)
    def _():
        main = main_summary()
        total[pl.ds(main_rows, TAIL * per_chunk), :] = piece_total(half_blocks)
        for slot in range(ny):
            far_copy(0, slot).wait_recv()
        far = functools.reduce(jnp.add, [far_tail[slot] for slot in range(ny)])
        blocks = [total[pl.ds(main_rows, TAIL * per_chunk), :], far.reshape(-1, query_count)]
        far_stat.wait_recv()
        stats[gx] = pair(*joined([main, summary(blocks), read(nx)]))
        share("gx", 0, gx, nx, gx)
        for turn in range(1, nx):
            stat_copy("gx", 0, gx, nx, lax.rem(gx + turn, nx), turn).wait_recv()
        stats[nx + 1] = pair(*joined([read(slot) for slot in range(nx)]))
        share("gz", nx, gz, nz, 1)

    @pl.when(jnp.logical_not(first))
    def _():
        final_stat.wait_recv()

    top, summed = read(nx + 1)
    scores = total[...]
    out_tile[...] = (scores - (top + jnp.log(summed))).T
    result = pltpu.make_async_copy(out_tile, out, out_sem)
    result.start()

    for flow in flows:
        @pl.when(jnp.logical_not(flow.is_last))
        def _():
            whole = pl.ds(0, chunks)
            pltpu.make_async_remote_copy(
                src_ref=flow.got.at[whole],
                dst_ref=flow.got.at[whole],
                send_sem=z_send.at[flow.index],
                recv_sem=flow.recv.at[0],
                device_id={"gz": flow.target},
                device_id_type=MESH,
            ).wait_send()

    @pl.when(at_end)
    def _():
        for turn in range(1, ny):
            peer_copy(turn, gy, 0, (pl.ds(0, chunks),)).wait_send()
        for block in range(half_blocks - 1):
            forward_copy(block).wait_send()

    @pl.when(last)
    def _():
        for turn in range(ny):
            far_copy(turn, gy).wait_send()
        far_stat.wait_send()

    @pl.when(first)
    def _():
        for axis, base, place, count, slot in (("gx", 0, gx, nx, gx), ("gz", nx, gz, nz, 1)):
            for turn in range(1, count):
                stat_copy(axis, base, place, count, slot, turn).wait_send()

    result.wait()


def shards(sizes, queries, passages, passage_len, query_len):
    nx, ny, nz = sizes
    query_count, query_rows, width = queries.shape
    passage_count, token_count, _ = passages.shape
    row_count = query_count * query_rows
    block_rows = passage_count // nz
    per_chunk = PER_CHUNK
    chunks = passage_count // 2 // per_chunk
    half_blocks = nz // 2
    maxima = pltpu.VMEM((chunks + 1, per_chunk, row_count), jnp.float32)
    dma = pltpu.SemaphoreType.DMA
    anywhere = pl.BlockSpec(memory_space=pltpu.HBM)
    return pl.pallas_call(
        functools.partial(kernel, sizes),
        out_shape=jax.ShapeDtypeStruct((query_count, block_rows), jnp.float32),
        in_specs=[anywhere] * 4,
        out_specs=anywhere,
        scratch_shapes=[
            pltpu.VMEM(queries.shape, queries.dtype),
            pltpu.VMEM((passage_count // 128, 128), passage_len.dtype),
            pltpu.VMEM((1, query_count), query_len.dtype),
            pltpu.VMEM(passages.shape, passages.dtype),
            pltpu.VMEM((2 * per_chunk * token_count, width), jnp.bfloat16),
            pltpu.VMEM((row_count, width), jnp.float32),
            pltpu.VMEM((width, row_count), jnp.bfloat16),
            pltpu.VMEM((passage_count, 128), jnp.float32),
            maxima,
            maxima,
            maxima,
            maxima,
            pltpu.VMEM((ny, chunks, per_chunk, query_count), jnp.float32),
            pltpu.VMEM((max(1, half_blocks - 1), block_rows, query_count), jnp.float32),
            pltpu.VMEM((block_rows, query_count), jnp.float32),
            pltpu.VMEM((nx + 2, 8, query_count), jnp.float32),
            pltpu.VMEM((ny, TAIL, per_chunk, query_count), jnp.float32),
            pltpu.VMEM((query_count, block_rows), jnp.float32),
            dma((3,)),
            dma((2 * chunks,)),
            dma((2,)),
            dma,
            dma((chunks,)),
            dma((chunks,)),
            dma((ny,)),
            dma((ny, half_blocks + 1)),
            dma((max(1, half_blocks - 1),)),
            dma,
            dma((nx + nz,)),
            dma((nx + nz,)),
            dma((ny,)),
            dma((ny,)),
        ],
        compiler_params=pltpu.CompilerParams(
            collective_id=0, has_side_effects=True, vmem_limit_bytes=67043328
        ),
    )(
        queries,
        passage_len.reshape(passage_count // 128, 128),
        query_len.reshape(1, query_count),
        passages,
    )


def solution(mesh):
    sizes = tuple(mesh.shape[name] for name in ("gx", "gy", "gz"))
    return jax.shard_map(
        functools.partial(shards, sizes),
        mesh=mesh,
        in_specs=(P(None, "gy", None), P("gx", "gz", None), P("gx"), P()),
        out_specs=P(None, ("gx", "gz")),
        check_vma=False,
    )
```

```python
import functools

import jax
import jax.numpy as jnp
from jax import lax
from jax.experimental import pallas as pl
from jax.experimental.pallas import tpu as pltpu
from jax.sharding import PartitionSpec as P

masked_low = -1e30
MESH = pl.DeviceIdType.MESH
UP_LAGS = ((3, 3), (2, 2), (3, 3), (2, 2))
DOWN_LAGS = ((4, 3), (3, 2), (4, 3), (3, 2))
TAIL_PARTS = 2
PEER_LAG = 3
TAIL = 2
VMEM_BYTES = 67043328
PER_CHUNK = 16


def kernel(
    sizes,
    queries_in,
    lengths_in,
    query_len_in,
    passages,
    out,
    queries,
    lengths,
    query_len,
    x,
    masked_x,
    wide_queries,
    query_columns,
    limits,
    own,
    got,
    partials,
    forward,
    total,
    stats,
    far_tail,
    small_sem,
    load_sem,
    z_send,
    z_recv,
    peer_send,
    peer_recv,
    forward_send,
    forward_recv,
    stat_send,
    stat_recv,
    far_send,
    far_recv,
):
    nx, ny, nz = sizes
    gx, gy, gz = (lax.axis_index(name) for name in ("gx", "gy", "gz"))
    passage_count, token_count, width = x.shape
    query_count, query_rows, _ = queries.shape
    _, chunks, per_chunk, row_count = own.shape
    tail_rows = per_chunk // TAIL_PARTS
    half_blocks = nz // 2
    per_block = chunks // half_blocks
    block_rows = passage_count // nz

    def low_start(c):
        return (half_blocks - 1 - c // per_block) * block_rows + (c % per_block) * per_chunk

    def high_start(c):
        return half_blocks * block_rows + c * per_chunk

    small = [
        pltpu.make_async_copy(source, target, small_sem.at[index])
        for index, (source, target) in enumerate(
            ((queries_in, queries), (lengths_in, lengths), (query_len_in, query_len))
        )
    ]
    for copy in small:
        copy.start()

    barrier = pltpu.get_barrier_semaphore()
    for axis, place, count in (("gx", gx, nx), ("gy", gy, ny)):
        for turn in range(1, count):
            pl.semaphore_signal(
                barrier,
                inc=1,
                device_id={axis: lax.rem(place + turn, count)},
                device_id_type=MESH,
            )
    for has_neighbour, neighbour in ((gz > 0, gz - 1), (gz < nz - 1, gz + 1)):
        @pl.when(has_neighbour)
        def _():
            pl.semaphore_signal(
                barrier, inc=1, device_id={"gz": neighbour}, device_id_type=MESH
            )

    at_end = (gz == 0) | (gz == nz - 1)

    def load(start, rows, group):
        rows = pl.ds(start, rows)
        return pltpu.make_async_copy(passages.at[rows], x.at[rows], load_sem.at[group])

    group_rows = (per_chunk, block_rows - per_chunk) + (block_rows,) * (half_blocks - 1)
    for group, rows in enumerate(group_rows):
        c = group if group < 2 else (group - 1) * per_block
        load(low_start(c), rows, group).start()
        load(high_start(c), rows, group).start()

    def wait_load(group):
        load(0, 2 * group_rows[group], group).wait()

    for copy in small:
        copy.wait()

    wide_queries[...] = queries[...].astype(jnp.float32).reshape(row_count, width)
    for i in range(query_rows):
        tile = wide_queries[pl.ds(i, query_count, stride=query_rows), :]
        query_columns[:, i * query_count : (i + 1) * query_count] = tile.T.astype(jnp.bfloat16)

    first_token = (gz * token_count).astype(jnp.float32)
    for b in range(passage_count // 128):
        row = lengths[b : b + 1, :].astype(jnp.float32) - first_token
        limits[b * 128 : (b + 1) * 128, :] = jnp.broadcast_to(row, (128, 128)).T

    token_ids = lax.broadcasted_iota(jnp.int32, (token_count, width), 0).astype(jnp.float32)
    tile_columns = 256

    def compute(c, sides):
        rows = len(sides) * per_chunk
        limit = []
        for place, side in enumerate(sides):
            start = jnp.where(side == 0, low_start(c), high_start(c))
            for p in range(per_chunk):
                tokens = x[start + p].astype(jnp.float32)
                usable = token_ids < limits[pl.ds(start + p, 1), :]
                tokens = jnp.where(usable, tokens, tokens[0:1, :])
                row = (place * per_chunk + p) * token_count
                masked_x[row : row + token_count, :] = tokens.astype(jnp.bfloat16)
            limit.append(limits[pl.ds(start, per_chunk), :])
        limit = jnp.concatenate(limit, axis=0)
        any_used = jnp.concatenate([limit] * (tile_columns // 128), axis=1) > 0.0
        for t in range(row_count // tile_columns):
            columns = slice(t * tile_columns, (t + 1) * tile_columns)
            scores = jnp.dot(
                masked_x[0 : rows * token_count, :],
                query_columns[:, columns],
                preferred_element_type=jnp.float32,
            )
            best = jnp.max(scores.reshape(rows, token_count, tile_columns), axis=1)
            best = jnp.where(any_used, best, masked_low)
            for place, side in enumerate(sides):
                own[side, c, :, columns] = best[place * per_chunk : (place + 1) * per_chunk]

    class Flow:
        def __init__(self, side, hops, lags, target):
            self.side, self.target = side, target
            self.is_first, self.is_last = hops == 0, hops == nz - 1
            self.is_inner = (hops > 0) & (hops < nz - 1)
            even, odd, late_even, late_odd = (start + more * (hops - 1) for start, more in lags)
            self.lag = jnp.where(
                lax.rem(gx, 2) == 0,
                jnp.where(gy == 0, even, late_even),
                jnp.where(gy == 0, odd, late_odd),
            )

        def copy(self, source, where, index):
            return pltpu.make_async_remote_copy(
                src_ref=source.at[(self.side, *where)],
                dst_ref=got.at[(self.side, *where)],
                send_sem=z_send.at[self.side],
                recv_sem=z_recv.at[self.side, index],
                device_id={"gz": self.target},
                device_id_type=MESH,
            )

        def merge(self, where):
            where = (self.side, *where)
            got[where] = jnp.maximum(got[where], own[where])

    def pieces(c, act):
        @pl.when(c < chunks - 1)
        def _():
            act((c,), c)

        @pl.when(c == chunks - 1)
        def _():
            for part in range(TAIL_PARTS):
                act((c, pl.ds(part * tail_rows, tail_rows)), c + part)

    first, last = gz == 0, gz == nz - 1
    below, above = lax.rem(gz + nz - 1, nz), lax.rem(gz + 1, nz)
    low = Flow(0, nz - 1 - gz, DOWN_LAGS, below)
    high = Flow(1, gz, UP_LAGS, above)
    flows = (low, high)

    def peer_copy(turn, slot, block, where):
        return pltpu.make_async_remote_copy(
            src_ref=partials.at[(slot, *where)],
            dst_ref=partials.at[(slot, *where)],
            send_sem=peer_send,
            recv_sem=peer_recv.at[slot, block],
            device_id={"gy": lax.rem(gy + turn, ny)},
            device_id_type=MESH,
        )

    def finalise(side, c):
        counted = query_len[...] - gy * query_rows
        so_far = jnp.zeros((per_chunk, query_count), jnp.float32)
        for i in range(query_rows):
            values = got[side, c, :, i * query_count : (i + 1) * query_count]
            so_far = so_far + jnp.where(counted > i, values, 0.0)
        partials[gy, c] = so_far

        @pl.when(last & (c >= chunks - TAIL))
        def _():
            for turn in reversed(range(ny)):
                far_copy(turn, gy, c - (chunks - TAIL)).start()

        for turn in range(1, ny):
            peer_copy(turn, gy, piece_of(c), (c,)).start()

    def piece_of(c):
        return c // per_block + jnp.where(c >= chunks - TAIL, 1, 0)

    def piece_total(piece):
        start = piece * per_block if piece < half_blocks else chunks - TAIL
        count = TAIL if piece == half_blocks else per_block - TAIL * (piece == half_blocks - 1)
        where = pl.ds(start, count)
        for turn in range(1, ny):
            slot = lax.rem(gy + turn, ny)
            peer_copy(turn, slot, piece, (where,)).wait_recv()
        summed = partials[0, where]
        for slot in range(1, ny):
            summed = summed + partials[slot, where]
        return summed.reshape(count * per_chunk, query_count)

    def far_copy(turn, slot, piece):
        return pltpu.make_async_remote_copy(
            src_ref=partials.at[slot, chunks - TAIL + piece],
            dst_ref=far_tail.at[slot, piece],
            send_sem=far_send,
            recv_sem=far_recv.at[slot, piece],
            device_id={"gy": lax.rem(gy + turn, ny), "gz": 0},
            device_id_type=MESH,
        )

    def forward_copy(block):
        target = jnp.where(gz == 0, half_blocks - 1 - block, half_blocks + block)
        return pltpu.make_async_remote_copy(
            src_ref=forward.at[block],
            dst_ref=total,
            send_sem=forward_send.at[block],
            recv_sem=forward_recv,
            device_id={"gz": target},
            device_id_type=MESH,
        )

    def pass_on(s):
        for flow in flows:
            c = s - flow.lag

            @pl.when(flow.is_inner & (c >= 0) & (c < chunks))
            def _():
                def act(where, index):
                    flow.copy(got, where, index).wait_recv()
                    flow.merge(where)
                    flow.copy(got, where, index).start()

                pieces(c, act)

    def send(c):
        for flow in flows:
            @pl.when(flow.is_first)
            def _():
                pieces(c, lambda where, index: flow.copy(own, where, index).start())

    def step(s, carry):
        pass_on(s)
        for group in range(1, len(group_rows)):
            @pl.when(s == (1 if group == 1 else (group - 1) * per_block))
            def _():
                wait_load(group)

        compute(s, (0, 1))
        send(s)
        return carry

    def drain(s, carry):
        pass_on(s)
        return carry

    urgent = jnp.where(gz < half_blocks, 1, 0)
    wait_load(0)
    compute(0, (urgent,))
    pl.semaphore_wait(barrier, nx + ny - 2 + jnp.where(at_end, 1, 2))
    send(0)
    compute(0, (1 - urgent,))
    lax.fori_loop(1, chunks, step, 0)

    @pl.when(jnp.logical_not(at_end))
    def _():
        last_lag = max(start + more * (nz - 3) for start, more in UP_LAGS + DOWN_LAGS)
        lax.fori_loop(chunks, chunks + last_lag, drain, 0)

    for flow in flows:
        @pl.when(flow.is_last)
        def _():
            def collect(c, carry):
                def act(where, index):
                    flow.copy(got, where, index).wait_recv()
                    flow.merge(where)

                pieces(c, act)
                finalise(flow.side, c)
                for block in range(half_blocks - 1):
                    @pl.when(c == (block + 1) * per_block - 1 + PEER_LAG)
                    def _():
                        forward[block] = piece_total(block)
                        forward_copy(block).start()
                return carry

            lax.fori_loop(0, chunks, collect, 0)

    main_rows = block_rows - TAIL * per_chunk
    row_ids = lax.broadcasted_iota(jnp.int32, stats.shape[1:], 0)

    def stat_copy(slot, to_x, to_z):
        return pltpu.make_async_remote_copy(
            src_ref=stats.at[slot],
            dst_ref=stats.at[slot],
            send_sem=stat_send,
            recv_sem=stat_recv.at[slot],
            device_id={"gx": to_x, "gz": to_z},
            device_id_type=MESH,
        )

    def pair(top, summed):
        return jnp.where(row_ids == 0, top, summed)

    def joined(pairs):
        highest = functools.reduce(jnp.maximum, [top for top, _ in pairs])
        shares = [summed * jnp.exp(top - highest) for top, summed in pairs]
        return highest, functools.reduce(jnp.add, shares)

    def summary(blocks):
        tops = [jnp.max(block, axis=0, keepdims=True) for block in blocks]
        top = functools.reduce(jnp.maximum, tops)
        sums = [jnp.sum(jnp.exp(block - top), axis=0, keepdims=True) for block in blocks]
        return top, functools.reduce(jnp.add, sums)

    def read(slot):
        return stats[slot, 0:1, :], stats[slot, 1:2, :]

    def main_summary():
        total[pl.ds(0, main_rows), :] = piece_total(half_blocks - 1)
        blocks = [forward[block] for block in range(half_blocks - 1)]
        return summary(blocks + [total[pl.ds(0, main_rows), :]])

    far_stat = stat_copy(nx, gx, 0)

    @pl.when(last)
    def _():
        stats[nx] = pair(*main_summary())
        far_stat.start()
        total[pl.ds(main_rows, TAIL * per_chunk), :] = piece_total(half_blocks)

    @pl.when(jnp.logical_not(at_end))
    def _():
        forward_copy(0).wait_recv()

    @pl.when(first)
    def _():
        main = main_summary()
        total[pl.ds(main_rows, TAIL * per_chunk), :] = piece_total(half_blocks)
        for slot in range(ny):
            for piece in range(TAIL):
                far_copy(0, slot, piece).wait_recv()
        far = functools.reduce(jnp.add, [far_tail[slot] for slot in range(ny)])
        blocks = [total[pl.ds(main_rows, TAIL * per_chunk), :], far.reshape(-1, query_count)]
        far_stat.wait_recv()
        stats[gx] = pair(*joined([main, summary(blocks), read(nx)]))
        for turn in range(1, nx * nz):
            stat_copy(gx, lax.rem(gx + turn % nx, nx), turn // nx).start()
        for turn in range(1, nx):
            stat_copy(lax.rem(gx + turn, nx), gx, gz).wait_recv()

    @pl.when(jnp.logical_not(first))
    def _():
        for slot in range(nx):
            stat_copy(slot, gx, gz).wait_recv()

    top, summed = joined([read(slot) for slot in range(nx)])
    scores = total[...]
    out[...] = (scores - (top + jnp.log(summed))).T

    def wait_sent(whole, sem):
        pltpu.make_async_remote_copy(
            src_ref=whole,
            dst_ref=whole,
            send_sem=sem,
            recv_sem=forward_recv,
            device_id={"gz": below},
            device_id_type=MESH,
        ).wait_send()

    for flow in flows:
        @pl.when(jnp.logical_not(flow.is_last))
        def _():
            wait_sent(got.at[flow.side], z_send.at[flow.side])

    @pl.when(at_end)
    def _():
        wait_sent(partials.at[pl.ds(0, ny - 1)], peer_send)
        for block in range(half_blocks - 1):
            forward_copy(block).wait_send()

    @pl.when(last)
    def _():
        wait_sent(far_tail, far_send)
        far_stat.wait_send()

    @pl.when(first)
    def _():
        wait_sent(stats.at[pl.ds(0, nx * nz - 1)], stat_send)


def shards(sizes, queries, passages, passage_len, query_len):
    nx, ny, nz = sizes
    query_count, query_rows, width = queries.shape
    passage_count, token_count, _ = passages.shape
    row_count = query_count * query_rows
    block_rows = passage_count // nz
    per_chunk = PER_CHUNK
    chunks = passage_count // 2 // per_chunk
    half_blocks = nz // 2
    maxima = pltpu.VMEM((2, chunks, per_chunk, row_count), jnp.float32)
    dma = pltpu.SemaphoreType.DMA
    anywhere = pl.BlockSpec(memory_space=pltpu.HBM)
    return pl.pallas_call(
        functools.partial(kernel, sizes),
        out_shape=pltpu.VMEM((query_count, block_rows), jnp.float32),
        in_specs=[anywhere] * 4,
        out_specs=pl.BlockSpec(memory_space=pltpu.VMEM),
        scratch_shapes=[
            pltpu.VMEM(queries.shape, queries.dtype),
            pltpu.VMEM((passage_count // 128, 128), passage_len.dtype),
            pltpu.VMEM((1, query_count), query_len.dtype),
            pltpu.VMEM(passages.shape, passages.dtype),
            pltpu.VMEM((2 * per_chunk * token_count, width), jnp.bfloat16),
            pltpu.VMEM((row_count, width), jnp.float32),
            pltpu.VMEM((width, row_count), jnp.bfloat16),
            pltpu.VMEM((passage_count, 128), jnp.float32),
            maxima,
            maxima,
            pltpu.VMEM((ny, chunks, per_chunk, query_count), jnp.float32),
            pltpu.VMEM((max(1, half_blocks - 1), block_rows, query_count), jnp.float32),
            pltpu.VMEM((block_rows, query_count), jnp.float32),
            pltpu.VMEM((max(nx + 1, nx * nz - 1), 8, query_count), jnp.float32),
            pltpu.VMEM((ny, TAIL, per_chunk, query_count), jnp.float32),
            dma((3,)),
            dma((half_blocks + 1,)),
            dma((2,)),
            dma((2, chunks + TAIL_PARTS - 1)),
            dma,
            dma((ny, half_blocks + 1)),
            dma((max(1, half_blocks - 1),)),
            dma,
            dma,
            dma((nx + 1,)),
            dma,
            dma((ny, TAIL)),
        ],
        compiler_params=pltpu.CompilerParams(
            collective_id=0, has_side_effects=True, vmem_limit_bytes=VMEM_BYTES - 4 * query_count * block_rows
        ),
    )(
        queries,
        passage_len.reshape(passage_count // 128, 128),
        query_len.reshape(1, query_count),
        passages,
    )


def solution(mesh):
    sizes = tuple(mesh.shape[name] for name in ("gx", "gy", "gz"))
    return jax.shard_map(
        functools.partial(shards, sizes),
        mesh=mesh,
        in_specs=(P(None, "gy", None), P("gx", "gz", None), P("gx"), P()),
        out_specs=P(None, ("gx", "gz")),
        check_vma=False,
    )
```

```python
import functools

import jax
import jax.numpy as jnp
from jax import lax
from jax.experimental import pallas as pl
from jax.experimental.pallas import tpu as pltpu
from jax.sharding import PartitionSpec as P

masked_low = -1e30
MESH = pl.DeviceIdType.MESH
UP_LAGS = ((3, 3), (2, 2))
DOWN_LAGS = ((4, 3), (3, 2))
TAIL_PARTS = 2
PEER_LAG = 3
TAIL = 2
VMEM_BYTES = 67043328
PER_CHUNK = 16


def kernel(
    sizes,
    queries_in,
    lengths_in,
    query_len_in,
    passages,
    out,
    queries,
    lengths,
    query_len,
    x,
    masked_x,
    wide_queries,
    query_columns,
    limits,
    own,
    got,
    partials,
    forward,
    total,
    stats,
    far_tail,
    small_sem,
    load_sem,
    z_send,
    z_recv,
    peer_send,
    peer_recv,
    forward_send,
    forward_recv,
    stat_send,
    stat_recv,
    far_send,
    far_recv,
):
    nx, ny, nz = sizes
    gx, gy, gz = (lax.axis_index(name) for name in ("gx", "gy", "gz"))
    passage_count, token_count, width = x.shape
    query_count, query_rows, _ = queries.shape
    _, chunks, per_chunk, row_count = own.shape
    tail_rows = per_chunk // TAIL_PARTS
    half_blocks = nz // 2
    per_block = chunks // half_blocks
    block_rows = passage_count // nz

    def low_start(c):
        return (half_blocks - 1 - c // per_block) * block_rows + (c % per_block) * per_chunk

    def high_start(c):
        return half_blocks * block_rows + c * per_chunk

    small = [
        pltpu.make_async_copy(source, target, small_sem.at[index])
        for index, (source, target) in enumerate(
            ((queries_in, queries), (lengths_in, lengths), (query_len_in, query_len))
        )
    ]
    for copy in small:
        copy.start()

    barrier = pltpu.get_barrier_semaphore()
    for axis, place, count in (("gx", gx, nx), ("gy", gy, ny)):
        for turn in range(1, count):
            pl.semaphore_signal(
                barrier,
                inc=1,
                device_id={axis: lax.rem(place + turn, count)},
                device_id_type=MESH,
            )
    for has_neighbour, neighbour in ((gz > 0, gz - 1), (gz < nz - 1, gz + 1)):
        @pl.when(has_neighbour)
        def _():
            pl.semaphore_signal(
                barrier, inc=1, device_id={"gz": neighbour}, device_id_type=MESH
            )

    at_end = (gz == 0) | (gz == nz - 1)

    def load(start, rows, group):
        rows = pl.ds(start, rows)
        return pltpu.make_async_copy(passages.at[rows], x.at[rows], load_sem.at[group])

    group_rows = (per_chunk, block_rows - per_chunk) + (block_rows,) * (half_blocks - 1)
    for group, rows in enumerate(group_rows):
        c = group if group < 2 else (group - 1) * per_block
        load(low_start(c), rows, group).start()
        load(high_start(c), rows, group).start()

    def wait_load(group):
        load(0, 2 * group_rows[group], group).wait()

    for copy in small[1:]:
        copy.wait()

    first_token = (gz * token_count).astype(jnp.float32)
    for b in range(passage_count // 128):
        row = lengths[b : b + 1, :].astype(jnp.float32) - first_token
        limits[b * 128 : (b + 1) * 128, :] = jnp.broadcast_to(row, (128, 128)).T

    small[0].wait()
    wide_queries[...] = queries[...].astype(jnp.float32).reshape(row_count, width)
    for i in range(query_rows):
        tile = wide_queries[pl.ds(i, query_count, stride=query_rows), :]
        query_columns[:, i * query_count : (i + 1) * query_count] = tile.T.astype(jnp.bfloat16)

    token_ids = lax.broadcasted_iota(jnp.int32, (token_count, width), 0).astype(jnp.float32)
    tile_columns = 256

    def compute(c, sides):
        rows = len(sides) * per_chunk
        limit = []
        for place, side in enumerate(sides):
            start = jnp.where(side == 0, low_start(c), high_start(c))
            for p in range(per_chunk):
                tokens = x[start + p].astype(jnp.float32)
                usable = token_ids < limits[pl.ds(start + p, 1), :]
                tokens = jnp.where(usable, tokens, tokens[0:1, :])
                row = (place * per_chunk + p) * token_count
                masked_x[row : row + token_count, :] = tokens.astype(jnp.bfloat16)
            limit.append(limits[pl.ds(start, per_chunk), :])
        limit = jnp.concatenate(limit, axis=0)
        any_used = jnp.concatenate([limit] * (tile_columns // 128), axis=1) > 0.0
        for t in range(row_count // tile_columns):
            columns = slice(t * tile_columns, (t + 1) * tile_columns)
            scores = jnp.dot(
                masked_x[0 : rows * token_count, :],
                query_columns[:, columns],
                preferred_element_type=jnp.float32,
            )
            best = jnp.max(scores.reshape(rows, token_count, tile_columns), axis=1)
            best = jnp.where(any_used, best, masked_low)
            for place, side in enumerate(sides):
                own[side, c, :, columns] = best[place * per_chunk : (place + 1) * per_chunk]

    class Flow:
        def __init__(self, side, hops, lags, target):
            self.side, self.target = side, target
            self.is_first, self.is_last = hops == 0, hops == nz - 1
            self.is_inner = (hops > 0) & (hops < nz - 1)
            even, odd = (start + more * (hops - 1) for start, more in lags)
            self.lag = jnp.where(lax.rem(gx, 2) == 0, even, odd)

        def copy(self, source, where, index):
            return pltpu.make_async_remote_copy(
                src_ref=source.at[(self.side, *where)],
                dst_ref=got.at[(self.side, *where)],
                send_sem=z_send.at[self.side],
                recv_sem=z_recv.at[self.side, index],
                device_id={"gz": self.target},
                device_id_type=MESH,
            )

        def merge(self, where):
            where = (self.side, *where)
            got[where] = jnp.maximum(got[where], own[where])

    def pieces(c, act):
        @pl.when(c < chunks - 1)
        def _():
            act((c,), c)

        @pl.when(c == chunks - 1)
        def _():
            for part in range(TAIL_PARTS):
                act((c, pl.ds(part * tail_rows, tail_rows)), c + part)

    first, last = gz == 0, gz == nz - 1
    below, above = lax.rem(gz + nz - 1, nz), lax.rem(gz + 1, nz)
    low = Flow(0, nz - 1 - gz, DOWN_LAGS, below)
    high = Flow(1, gz, UP_LAGS, above)
    flows = (low, high)

    def peer_copy(turn, slot, block, where):
        return pltpu.make_async_remote_copy(
            src_ref=partials.at[(slot, *where)],
            dst_ref=partials.at[(slot, *where)],
            send_sem=peer_send,
            recv_sem=peer_recv.at[block],
            device_id={"gy": lax.rem(gy + turn, ny)},
            device_id_type=MESH,
        )

    def finalise(side, c):
        counted = query_len[...] - gy * query_rows
        so_far = jnp.zeros((per_chunk, query_count), jnp.float32)
        for i in range(query_rows):
            values = got[side, c, :, i * query_count : (i + 1) * query_count]
            so_far = so_far + jnp.where(counted > i, values, 0.0)
        partials[gy, c] = so_far

        @pl.when(last & (c >= chunks - TAIL))
        def _():
            for turn in reversed(range(ny)):
                far_copy(turn, gy, c - (chunks - TAIL)).start()

        for turn in range(1, ny):
            peer_copy(turn, gy, piece_of(c), (c,)).start()

    def wait_landed(whole, sem):
        pltpu.make_async_remote_copy(
            src_ref=whole,
            dst_ref=whole,
            send_sem=peer_send,
            recv_sem=sem,
            device_id={"gz": below},
            device_id_type=MESH,
        ).wait_recv()

    def piece_of(c):
        return c // per_block + jnp.where(c >= chunks - TAIL, 1, 0)

    def piece_total(piece):
        start = piece * per_block if piece < half_blocks else chunks - TAIL
        count = TAIL if piece == half_blocks else per_block - TAIL * (piece == half_blocks - 1)
        where = pl.ds(start, count)
        wait_landed(partials.at[pl.ds(0, ny - 1), where], peer_recv.at[piece])
        summed = partials[0, where]
        for slot in range(1, ny):
            summed = summed + partials[slot, where]
        return summed.reshape(count * per_chunk, query_count)

    def far_copy(turn, slot, piece):
        return pltpu.make_async_remote_copy(
            src_ref=partials.at[slot, chunks - TAIL + piece],
            dst_ref=far_tail.at[slot, piece],
            send_sem=far_send,
            recv_sem=far_recv,
            device_id={"gy": lax.rem(gy + turn, ny), "gz": 0},
            device_id_type=MESH,
        )

    def forward_copy(block):
        target = jnp.where(gz == 0, half_blocks - 1 - block, half_blocks + block)
        return pltpu.make_async_remote_copy(
            src_ref=forward.at[block],
            dst_ref=total,
            send_sem=forward_send.at[block],
            recv_sem=forward_recv,
            device_id={"gz": target},
            device_id_type=MESH,
        )

    def pass_on(s):
        for flow in flows:
            c = s - flow.lag

            @pl.when(flow.is_inner & (c >= 0) & (c < chunks))
            def _():
                def act(where, index):
                    flow.copy(got, where, index).wait_recv()
                    flow.merge(where)
                    flow.copy(got, where, index).start()

                pieces(c, act)

    def send(c):
        for flow in flows:
            @pl.when(flow.is_first)
            def _():
                pieces(c, lambda where, index: flow.copy(own, where, index).start())

    def step(s, carry):
        pass_on(s)
        for group in range(1, len(group_rows)):
            @pl.when(s == (1 if group == 1 else (group - 1) * per_block))
            def _():
                wait_load(group)

        compute(s, (0, 1))
        send(s)
        return carry

    def drain(s, carry):
        pass_on(s)
        return carry

    urgent = jnp.where(gz < half_blocks, 1, 0)
    wait_load(0)
    compute(0, (urgent,))
    pl.semaphore_wait(barrier, nx + ny - 2 + jnp.where(at_end, 1, 2))
    send(0)
    compute(0, (1 - urgent,))
    lax.fori_loop(1, chunks, step, 0)

    @pl.when(jnp.logical_not(at_end))
    def _():
        last_lag = max(start + more * (nz - 3) for start, more in UP_LAGS + DOWN_LAGS)
        lax.fori_loop(chunks, chunks + last_lag, drain, 0)

    for flow in flows:
        @pl.when(flow.is_last)
        def _():
            def collect(c, carry):
                def act(where, index):
                    flow.copy(got, where, index).wait_recv()
                    flow.merge(where)

                pieces(c, act)
                finalise(flow.side, c)
                for block in range(half_blocks - 1):
                    @pl.when(c == (block + 1) * per_block - 1 + PEER_LAG)
                    def _():
                        forward[block] = piece_total(block)
                        forward_copy(block).start()
                return carry

            lax.fori_loop(0, chunks, collect, 0)

    main_rows = block_rows - TAIL * per_chunk
    row_ids = lax.broadcasted_iota(jnp.int32, stats.shape[1:], 0)

    def stat_copy(slot, to_x, to_y, to_z, kind=0):
        return pltpu.make_async_remote_copy(
            src_ref=stats.at[slot],
            dst_ref=stats.at[slot],
            send_sem=stat_send,
            recv_sem=stat_recv.at[kind],
            device_id={"gx": to_x, "gy": to_y, "gz": to_z},
            device_id_type=MESH,
        )

    def pair(top, summed):
        return jnp.where(row_ids == 0, top, summed)

    def joined(pairs):
        highest = functools.reduce(jnp.maximum, [top for top, _ in pairs])
        shares = [summed * jnp.exp(top - highest) for top, summed in pairs]
        return highest, functools.reduce(jnp.add, shares)

    def summary(blocks):
        tops = [jnp.max(block, axis=0, keepdims=True) for block in blocks]
        top = functools.reduce(jnp.maximum, tops)
        sums = [jnp.sum(jnp.exp(block - top), axis=0, keepdims=True) for block in blocks]
        return top, functools.reduce(jnp.add, sums)

    def read(slot):
        return stats[slot, 0:1, :], stats[slot, 1:2, :]

    def main_summary():
        total[pl.ds(0, main_rows), :] = piece_total(half_blocks - 1)
        blocks = [forward[block] for block in range(half_blocks - 1)]
        return summary(blocks + [total[pl.ds(0, main_rows), :]])

    far_stat = stat_copy(nx, gx, gy, 0, 1)
    beside = [lax.rem(gx + turn, nx) for turn in range(1, nx)]
    column = [(lax.rem(gx + turn, nx), to_z) for turn in range(nx) for to_z in range(1, nz)]
    helper = min(1, ny - 1)
    shared = (nx - 1, nx - 1 + len(column), nx - 1 + 2 * len(column))

    def shares(act):
        @pl.when((gy == 0) & (helper != 0))
        def _():
            act(0)

        @pl.when((gy != helper) & (gy != 0))
        def _():
            act(1)

        @pl.when(gy == helper)
        def _():
            act(2 if helper else 1)


    @pl.when(last)
    def _():
        stats[nx] = pair(*main_summary())
        far_stat.start()
        total[pl.ds(main_rows, TAIL * per_chunk), :] = piece_total(half_blocks)

    @pl.when(jnp.logical_not(at_end))
    def _():
        forward_copy(0).wait_recv()

    @pl.when(first)
    def _():
        main = main_summary()
        total[pl.ds(main_rows, TAIL * per_chunk), :] = piece_total(half_blocks)
        wait_landed(far_tail, far_recv)
        far = functools.reduce(jnp.add, [far_tail[slot] for slot in range(ny)])
        blocks = [total[pl.ds(main_rows, TAIL * per_chunk), :], far.reshape(-1, query_count)]
        far_stat.wait_recv()
        stats[gx] = pair(*joined([main, summary(blocks), read(nx)]))
        for to_x in beside:
            stat_copy(gx, to_x, gy, gz).start()

        def share(columns):
            for to_y in (gy, 0)[:columns]:
                for to_x, to_z in column:
                    stat_copy(gx, to_x, to_y, to_z).start()

        shares(share)
        wait_landed(stats.at[pl.ds(0, nx - 1)], stat_recv.at[0])

    @pl.when(jnp.logical_not(first))
    def _():
        wait_landed(stats.at[pl.ds(0, nx)], stat_recv.at[0])

    top, summed = joined([read(slot) for slot in range(nx)])
    scores = total[...]
    out[...] = (scores - (top + jnp.log(summed))).T

    def wait_sent(whole, sem):
        pltpu.make_async_remote_copy(
            src_ref=whole,
            dst_ref=whole,
            send_sem=sem,
            recv_sem=forward_recv,
            device_id={"gz": below},
            device_id_type=MESH,
        ).wait_send()

    for flow in flows:
        @pl.when(jnp.logical_not(flow.is_last))
        def _():
            wait_sent(got.at[flow.side], z_send.at[flow.side])

    @pl.when(at_end)
    def _():
        wait_sent(partials.at[pl.ds(0, ny - 1)], peer_send)
        for block in range(half_blocks - 1):
            forward_copy(block).wait_send()

    @pl.when(last)
    def _():
        wait_sent(far_tail, far_send)
        far_stat.wait_send()

    @pl.when(first)
    def _():
        shares(lambda columns: wait_sent(stats.at[pl.ds(0, shared[columns])], stat_send))


def shards(sizes, queries, passages, passage_len, query_len):
    nx, ny, nz = sizes
    query_count, query_rows, width = queries.shape
    passage_count, token_count, _ = passages.shape
    row_count = query_count * query_rows
    block_rows = passage_count // nz
    per_chunk = PER_CHUNK
    chunks = passage_count // 2 // per_chunk
    half_blocks = nz // 2
    maxima = pltpu.VMEM((2, chunks, per_chunk, row_count), jnp.float32)
    dma = pltpu.SemaphoreType.DMA
    anywhere = pl.BlockSpec(memory_space=pltpu.HBM)
    return pl.pallas_call(
        functools.partial(kernel, sizes),
        out_shape=pltpu.VMEM((query_count, block_rows), jnp.float32),
        in_specs=[anywhere] * 4,
        out_specs=pl.BlockSpec(memory_space=pltpu.VMEM),
        scratch_shapes=[
            pltpu.VMEM(queries.shape, queries.dtype),
            pltpu.VMEM((passage_count // 128, 128), passage_len.dtype),
            pltpu.VMEM((1, query_count), query_len.dtype),
            pltpu.VMEM(passages.shape, passages.dtype),
            pltpu.VMEM((2 * per_chunk * token_count, width), jnp.bfloat16),
            pltpu.VMEM((row_count, width), jnp.float32),
            pltpu.VMEM((width, row_count), jnp.bfloat16),
            pltpu.VMEM((passage_count, 128), jnp.float32),
            maxima,
            maxima,
            pltpu.VMEM((ny, chunks, per_chunk, query_count), jnp.float32),
            pltpu.VMEM((max(1, half_blocks - 1), block_rows, query_count), jnp.float32),
            pltpu.VMEM((block_rows, query_count), jnp.float32),
            pltpu.VMEM((nx * (2 * nz - 1), 8, query_count), jnp.float32),
            pltpu.VMEM((ny, TAIL, per_chunk, query_count), jnp.float32),
            dma((3,)),
            dma((half_blocks + 1,)),
            dma((2,)),
            dma((2, chunks + TAIL_PARTS - 1)),
            dma,
            dma((half_blocks + 1,)),
            dma((max(1, half_blocks - 1),)),
            dma,
            dma,
            dma((2,)),
            dma,
            dma,
        ],
        compiler_params=pltpu.CompilerParams(
            collective_id=0, has_side_effects=True, vmem_limit_bytes=VMEM_BYTES - 4 * query_count * block_rows
        ),
    )(
        queries,
        passage_len.reshape(passage_count // 128, 128),
        query_len.reshape(1, query_count),
        passages,
    )


def solution(mesh):
    sizes = tuple(mesh.shape[name] for name in ("gx", "gy", "gz"))
    return jax.shard_map(
        functools.partial(shards, sizes),
        mesh=mesh,
        in_specs=(P(None, "gy", None), P("gx", "gz", None), P("gx"), P()),
        out_specs=P(None, ("gx", "gz")),
        check_vma=False,
    )
```

```python
import functools

import jax
import jax.numpy as jnp
from jax import lax
from jax.experimental import pallas as pl
from jax.experimental.pallas import tpu as pltpu
from jax.sharding import PartitionSpec as P

masked_low = -1e30
MESH = pl.DeviceIdType.MESH
UP_LAGS = ((3, 3), (2, 2))
DOWN_LAGS = ((4, 3), (3, 2))
TAIL_PARTS = 2
PEER_LAG = 3
TAIL = 2
VMEM_BYTES = 67043328
PER_CHUNK = 16


def kernel(
    sizes,
    queries_in,
    lengths_in,
    query_len_in,
    passages,
    out,
    queries,
    lengths,
    query_len,
    x,
    masked_x,
    wide_queries,
    query_columns,
    limits,
    own,
    got,
    partials,
    forward,
    total,
    stats,
    far_tail,
    small_sem,
    load_sem,
    z_send,
    z_recv,
    peer_send,
    peer_recv,
    forward_send,
    forward_recv,
    stat_send,
    stat_recv,
    far_send,
    far_recv,
):
    nx, ny, nz = sizes
    gx, gy, gz = (lax.axis_index(name) for name in ("gx", "gy", "gz"))
    passage_count, token_count, width = x.shape
    query_count, query_rows, _ = queries.shape
    _, chunks, per_chunk, row_count = own.shape
    tail_rows = per_chunk // TAIL_PARTS
    half_blocks = nz // 2
    per_block = chunks // half_blocks
    block_rows = passage_count // nz

    def low_start(c):
        return (half_blocks - 1 - c // per_block) * block_rows + (c % per_block) * per_chunk

    def high_start(c):
        return half_blocks * block_rows + c * per_chunk

    small = [
        pltpu.make_async_copy(source, target, small_sem.at[index])
        for index, (source, target) in enumerate(
            ((queries_in, queries), (lengths_in, lengths), (query_len_in, query_len))
        )
    ]
    for copy in small:
        copy.start()

    barrier = pltpu.get_barrier_semaphore()
    for axis, place, count in (("gx", gx, nx), ("gy", gy, ny)):
        for turn in range(1, count):
            pl.semaphore_signal(
                barrier,
                inc=1,
                device_id={axis: lax.rem(place + turn, count)},
                device_id_type=MESH,
            )
    for has_neighbour, neighbour in ((gz > 0, gz - 1), (gz < nz - 1, gz + 1)):
        @pl.when(has_neighbour)
        def _():
            pl.semaphore_signal(
                barrier, inc=1, device_id={"gz": neighbour}, device_id_type=MESH
            )

    at_end = (gz == 0) | (gz == nz - 1)

    def load(start, rows, group):
        rows = pl.ds(start, rows)
        return pltpu.make_async_copy(passages.at[rows], x.at[rows], load_sem.at[group])

    group_rows = (per_chunk, block_rows - per_chunk) + (block_rows,) * (half_blocks - 1)
    for group, rows in enumerate(group_rows):
        c = group if group < 2 else (group - 1) * per_block
        load(low_start(c), rows, group).start()
        load(high_start(c), rows, group).start()

    def wait_load(group):
        load(0, 2 * group_rows[group], group).wait()

    for copy in small[1:]:
        copy.wait()

    first_token = (gz * token_count).astype(jnp.float32)
    for b in range(passage_count // 128):
        row = lengths[b : b + 1, :].astype(jnp.float32) - first_token
        limits[b * 128 : (b + 1) * 128, :] = jnp.broadcast_to(row, (128, 128)).T

    small[0].wait()
    wide_queries[...] = queries[...].astype(jnp.float32).reshape(row_count, width)
    for i in range(query_rows):
        tile = wide_queries[pl.ds(i, query_count, stride=query_rows), :]
        query_columns[:, i * query_count : (i + 1) * query_count] = tile.T.astype(jnp.bfloat16)

    token_ids = lax.broadcasted_iota(jnp.int32, (token_count, width), 0).astype(jnp.float32)
    tile_columns = 256

    def compute(*halves):
        rows = len(halves) * per_chunk
        limit = []
        for place, (side, c) in enumerate(halves):
            start = jnp.where(side == 0, low_start(c), high_start(c))
            for p in range(per_chunk):
                tokens = x[start + p].astype(jnp.float32)
                usable = token_ids < limits[pl.ds(start + p, 1), :]
                tokens = jnp.where(usable, tokens, tokens[0:1, :])
                row = (place * per_chunk + p) * token_count
                masked_x[row : row + token_count, :] = tokens.astype(jnp.bfloat16)
            limit.append(limits[pl.ds(start, per_chunk), :])
        limit = jnp.concatenate(limit, axis=0)
        any_used = jnp.concatenate([limit] * (tile_columns // 128), axis=1) > 0.0
        for t in range(row_count // tile_columns):
            columns = slice(t * tile_columns, (t + 1) * tile_columns)
            scores = jnp.dot(
                masked_x[0 : rows * token_count, :],
                query_columns[:, columns],
                preferred_element_type=jnp.float32,
            )
            best = jnp.max(scores.reshape(rows, token_count, tile_columns), axis=1)
            best = jnp.where(any_used, best, masked_low)
            for place, (side, c) in enumerate(halves):
                own[side, c, :, columns] = best[place * per_chunk : (place + 1) * per_chunk]

    class Flow:
        def __init__(self, side, hops, lags, target):
            self.side, self.target = side, target
            self.is_first, self.is_last = hops == 0, hops == nz - 1
            self.is_inner = (hops > 0) & (hops < nz - 1)
            even, odd = (start + more * (hops - 1) for start, more in lags)
            self.lag = jnp.where(lax.rem(gx, 2) == 0, even, odd)

        def copy(self, source, where, index):
            return pltpu.make_async_remote_copy(
                src_ref=source.at[(self.side, *where)],
                dst_ref=got.at[(self.side, *where)],
                send_sem=z_send.at[self.side],
                recv_sem=z_recv.at[self.side, index],
                device_id={"gz": self.target},
                device_id_type=MESH,
            )

        def merge(self, where):
            where = (self.side, *where)
            got[where] = jnp.maximum(got[where], own[where])

    def pieces(c, act):
        @pl.when(c < chunks - 1)
        def _():
            act((c,), c)

        @pl.when(c == chunks - 1)
        def _():
            for part in range(TAIL_PARTS):
                act((c, pl.ds(part * tail_rows, tail_rows)), c + part)

    first, last = gz == 0, gz == nz - 1
    below, above = lax.rem(gz + nz - 1, nz), lax.rem(gz + 1, nz)
    low = Flow(0, nz - 1 - gz, DOWN_LAGS, below)
    high = Flow(1, gz, UP_LAGS, above)
    flows = (low, high)

    def peer_copy(turn, slot, block, where):
        return pltpu.make_async_remote_copy(
            src_ref=partials.at[(slot, *where)],
            dst_ref=partials.at[(slot, *where)],
            send_sem=peer_send,
            recv_sem=peer_recv.at[block],
            device_id={"gy": lax.rem(gy + turn, ny)},
            device_id_type=MESH,
        )

    def finalise(side, c):
        counted = query_len[...] - gy * query_rows
        so_far = jnp.zeros((per_chunk, query_count), jnp.float32)
        for i in range(query_rows):
            values = got[side, c, :, i * query_count : (i + 1) * query_count]
            so_far = so_far + jnp.where(counted > i, values, 0.0)
        partials[gy, c] = so_far

        @pl.when(last & (c >= chunks - TAIL))
        def _():
            for turn in reversed(range(ny)):
                far_copy(turn, gy, c - (chunks - TAIL)).start()

        for turn in range(1, ny):
            peer_copy(turn, gy, piece_of(c), (c,)).start()

    def wait_landed(whole, sem):
        pltpu.make_async_remote_copy(
            src_ref=whole,
            dst_ref=whole,
            send_sem=peer_send,
            recv_sem=sem,
            device_id={"gz": below},
            device_id_type=MESH,
        ).wait_recv()

    def piece_of(c):
        return c // per_block + jnp.where(c >= chunks - TAIL, 1, 0)

    def piece_total(piece):
        start = piece * per_block if piece < half_blocks else chunks - TAIL
        count = TAIL if piece == half_blocks else per_block - TAIL * (piece == half_blocks - 1)
        where = pl.ds(start, count)
        wait_landed(partials.at[pl.ds(0, ny - 1), where], peer_recv.at[piece])
        summed = partials[0, where]
        for slot in range(1, ny):
            summed = summed + partials[slot, where]
        return summed.reshape(count * per_chunk, query_count)

    def far_copy(turn, slot, piece):
        return pltpu.make_async_remote_copy(
            src_ref=partials.at[slot, chunks - TAIL + piece],
            dst_ref=far_tail.at[slot, piece],
            send_sem=far_send,
            recv_sem=far_recv,
            device_id={"gy": lax.rem(gy + turn, ny), "gz": 0},
            device_id_type=MESH,
        )

    def forward_copy(block):
        target = jnp.where(gz == 0, half_blocks - 1 - block, half_blocks + block)
        return pltpu.make_async_remote_copy(
            src_ref=forward.at[block],
            dst_ref=total,
            send_sem=forward_send.at[block],
            recv_sem=forward_recv,
            device_id={"gz": target},
            device_id_type=MESH,
        )

    urgent = jnp.where(gz < half_blocks, 1, 0)

    def pass_on(s):
        for flow in flows:
            c = s - flow.lag

            @pl.when(flow.is_inner & (c >= 0) & (c < chunks))
            def _():
                def act(where, index):
                    flow.copy(got, where, index).wait_recv()
                    flow.merge(where)
                    flow.copy(got, where, index).start()

                pieces(c, act)

    def send(c):
        for flow in flows:
            @pl.when(flow.is_first)
            def _():
                pieces(c, lambda where, index: flow.copy(own, where, index).start())

    def step(s, carry):
        pass_on(s)
        for group in range(1, len(group_rows)):
            @pl.when(s == (1 if group == 1 else (group - 1) * per_block))
            def _():
                wait_load(group)

        compute((urgent, s), (1 - urgent, s - 1))
        send(s)
        return carry

    def drain(s, carry):
        pass_on(s)
        return carry

    wait_load(0)
    compute((urgent, 0))
    pl.semaphore_wait(barrier, nx + ny - 2 + jnp.where(at_end, 1, 2))
    send(0)
    lax.fori_loop(1, chunks, step, 0)
    pass_on(chunks)
    compute((1 - urgent, chunks - 1))

    @pl.when(jnp.logical_not(at_end))
    def _():
        last_lag = max(start + more * (nz - 3) for start, more in UP_LAGS + DOWN_LAGS)
        lax.fori_loop(chunks + 1, chunks + last_lag, drain, 0)

    for flow in flows:
        @pl.when(flow.is_last)
        def _():
            def collect(c, carry):
                def act(where, index):
                    flow.copy(got, where, index).wait_recv()
                    flow.merge(where)

                pieces(c, act)
                finalise(flow.side, c)
                for block in range(half_blocks - 1):
                    @pl.when(c == (block + 1) * per_block - 1 + PEER_LAG)
                    def _():
                        forward[block] = piece_total(block)
                        forward_copy(block).start()
                return carry

            lax.fori_loop(0, chunks, collect, 0)

    main_rows = block_rows - TAIL * per_chunk
    row_ids = lax.broadcasted_iota(jnp.int32, stats.shape[1:], 0)

    def stat_copy(slot, to_x, to_y, to_z, kind=0):
        return pltpu.make_async_remote_copy(
            src_ref=stats.at[slot],
            dst_ref=stats.at[slot],
            send_sem=stat_send,
            recv_sem=stat_recv.at[kind],
            device_id={"gx": to_x, "gy": to_y, "gz": to_z},
            device_id_type=MESH,
        )

    def pair(top, summed):
        return jnp.where(row_ids == 0, top, summed)

    def joined(pairs):
        highest = functools.reduce(jnp.maximum, [top for top, _ in pairs])
        shares = [summed * jnp.exp(top - highest) for top, summed in pairs]
        return highest, functools.reduce(jnp.add, shares)

    def summary(blocks):
        tops = [jnp.max(block, axis=0, keepdims=True) for block in blocks]
        top = functools.reduce(jnp.maximum, tops)
        sums = [jnp.sum(jnp.exp(block - top), axis=0, keepdims=True) for block in blocks]
        return top, functools.reduce(jnp.add, sums)

    def read(slot):
        return stats[slot, 0:1, :], stats[slot, 1:2, :]

    def main_summary():
        total[pl.ds(0, main_rows), :] = piece_total(half_blocks - 1)
        blocks = [forward[block] for block in range(half_blocks - 1)]
        return summary(blocks + [total[pl.ds(0, main_rows), :]])

    far_stat = stat_copy(nx, gx, gy, 0, 1)
    beside = [lax.rem(gx + turn, nx) for turn in range(1, nx)]
    column = [(lax.rem(gx + turn, nx), to_z) for turn in range(nx) for to_z in range(1, nz)]
    helper = min(1, ny - 1)
    shared = (nx - 1, nx - 1 + len(column), nx - 1 + 2 * len(column))

    def shares(act):
        @pl.when((gy == 0) & (helper != 0))
        def _():
            act(0)

        @pl.when((gy != helper) & (gy != 0))
        def _():
            act(1)

        @pl.when(gy == helper)
        def _():
            act(2 if helper else 1)


    @pl.when(last)
    def _():
        stats[nx] = pair(*main_summary())
        far_stat.start()
        total[pl.ds(main_rows, TAIL * per_chunk), :] = piece_total(half_blocks)

    @pl.when(jnp.logical_not(at_end))
    def _():
        forward_copy(0).wait_recv()

    @pl.when(first)
    def _():
        main = main_summary()
        total[pl.ds(main_rows, TAIL * per_chunk), :] = piece_total(half_blocks)
        wait_landed(far_tail, far_recv)
        far = functools.reduce(jnp.add, [far_tail[slot] for slot in range(ny)])
        blocks = [total[pl.ds(main_rows, TAIL * per_chunk), :], far.reshape(-1, query_count)]
        far_stat.wait_recv()
        stats[gx] = pair(*joined([main, summary(blocks), read(nx)]))
        for to_x in beside:
            stat_copy(gx, to_x, gy, gz).start()

        def share(columns):
            for to_y in (gy, 0)[:columns]:
                for to_x, to_z in column:
                    stat_copy(gx, to_x, to_y, to_z).start()

        shares(share)
        wait_landed(stats.at[pl.ds(0, nx - 1)], stat_recv.at[0])

    @pl.when(jnp.logical_not(first))
    def _():
        wait_landed(stats.at[pl.ds(0, nx)], stat_recv.at[0])

    top, summed = joined([read(slot) for slot in range(nx)])
    scores = total[...]
    out[...] = (scores - (top + jnp.log(summed))).T

    def wait_sent(whole, sem):
        pltpu.make_async_remote_copy(
            src_ref=whole,
            dst_ref=whole,
            send_sem=sem,
            recv_sem=forward_recv,
            device_id={"gz": below},
            device_id_type=MESH,
        ).wait_send()

    for flow in flows:
        @pl.when(jnp.logical_not(flow.is_last))
        def _():
            wait_sent(got.at[flow.side], z_send.at[flow.side])

    @pl.when(at_end)
    def _():
        wait_sent(partials.at[pl.ds(0, ny - 1)], peer_send)
        for block in range(half_blocks - 1):
            forward_copy(block).wait_send()

    @pl.when(last)
    def _():
        wait_sent(far_tail, far_send)
        far_stat.wait_send()

    @pl.when(first)
    def _():
        shares(lambda columns: wait_sent(stats.at[pl.ds(0, shared[columns])], stat_send))


def shards(sizes, queries, passages, passage_len, query_len):
    nx, ny, nz = sizes
    query_count, query_rows, width = queries.shape
    passage_count, token_count, _ = passages.shape
    row_count = query_count * query_rows
    block_rows = passage_count // nz
    per_chunk = PER_CHUNK
    chunks = passage_count // 2 // per_chunk
    half_blocks = nz // 2
    maxima = pltpu.VMEM((2, chunks, per_chunk, row_count), jnp.float32)
    dma = pltpu.SemaphoreType.DMA
    anywhere = pl.BlockSpec(memory_space=pltpu.HBM)
    return pl.pallas_call(
        functools.partial(kernel, sizes),
        out_shape=pltpu.VMEM((query_count, block_rows), jnp.float32),
        in_specs=[anywhere] * 4,
        out_specs=pl.BlockSpec(memory_space=pltpu.VMEM),
        scratch_shapes=[
            pltpu.VMEM(queries.shape, queries.dtype),
            pltpu.VMEM((passage_count // 128, 128), passage_len.dtype),
            pltpu.VMEM((1, query_count), query_len.dtype),
            pltpu.VMEM(passages.shape, passages.dtype),
            pltpu.VMEM((2 * per_chunk * token_count, width), jnp.bfloat16),
            pltpu.VMEM((row_count, width), jnp.float32),
            pltpu.VMEM((width, row_count), jnp.bfloat16),
            pltpu.VMEM((passage_count, 128), jnp.float32),
            maxima,
            maxima,
            pltpu.VMEM((ny, chunks, per_chunk, query_count), jnp.float32),
            pltpu.VMEM((max(1, half_blocks - 1), block_rows, query_count), jnp.float32),
            pltpu.VMEM((block_rows, query_count), jnp.float32),
            pltpu.VMEM((nx * (2 * nz - 1), 8, query_count), jnp.float32),
            pltpu.VMEM((ny, TAIL, per_chunk, query_count), jnp.float32),
            dma((3,)),
            dma((half_blocks + 1,)),
            dma((2,)),
            dma((2, chunks + TAIL_PARTS - 1)),
            dma,
            dma((half_blocks + 1,)),
            dma((max(1, half_blocks - 1),)),
            dma,
            dma,
            dma((2,)),
            dma,
            dma,
        ],
        compiler_params=pltpu.CompilerParams(
            collective_id=0, has_side_effects=True, vmem_limit_bytes=VMEM_BYTES - 4 * query_count * block_rows
        ),
    )(
        queries,
        passage_len.reshape(passage_count // 128, 128),
        query_len.reshape(1, query_count),
        passages,
    )


def solution(mesh):
    sizes = tuple(mesh.shape[name] for name in ("gx", "gy", "gz"))
    return jax.shard_map(
        functools.partial(shards, sizes),
        mesh=mesh,
        in_specs=(P(None, "gy", None), P("gx", "gz", None), P("gx"), P()),
        out_specs=P(None, ("gx", "gz")),
        check_vma=False,
    )
```

```python
import functools

import jax
import jax.numpy as jnp
from jax import lax
from jax.experimental import pallas as pl
from jax.experimental.pallas import tpu as pltpu
from jax.sharding import PartitionSpec as P

masked_low = -1e30
MESH = pl.DeviceIdType.MESH
UP_LAGS = ((3, 3), (2, 2))
DOWN_LAGS = ((4, 3), (3, 2))
TAIL_PARTS = 2
PEER_LAG = 3
TAIL = 2
VMEM_BYTES = 67043328
PER_CHUNK = 16


def kernel(
    sizes,
    queries_in,
    lengths_in,
    query_len_in,
    passages,
    out,
    queries,
    lengths,
    query_len,
    x,
    masked_x,
    wide_queries,
    query_columns,
    limits,
    own,
    got,
    partials,
    forward,
    total,
    stats,
    far_tail,
    small_sem,
    load_sem,
    z_send,
    z_recv,
    peer_send,
    peer_recv,
    forward_send,
    forward_recv,
    stat_send,
    stat_recv,
    far_send,
    far_recv,
):
    nx, ny, nz = sizes
    gx, gy, gz = (lax.axis_index(name) for name in ("gx", "gy", "gz"))
    passage_count, token_count, width = x.shape
    query_count, query_rows, _ = queries.shape
    _, chunks, per_chunk, row_count = own.shape
    tail_rows = per_chunk // TAIL_PARTS
    half_blocks = nz // 2
    per_block = chunks // half_blocks
    block_rows = passage_count // nz

    def low_start(c):
        return (half_blocks - 1 - c // per_block) * block_rows + (c % per_block) * per_chunk

    def high_start(c):
        return half_blocks * block_rows + c * per_chunk

    small = [
        pltpu.make_async_copy(source, target, small_sem.at[index])
        for index, (source, target) in enumerate(
            ((queries_in, queries), (lengths_in, lengths), (query_len_in, query_len))
        )
    ]
    for copy in small:
        copy.start()

    barrier = pltpu.get_barrier_semaphore()
    for axis, place, count in (("gx", gx, nx), ("gy", gy, ny)):
        for turn in range(1, count):
            pl.semaphore_signal(
                barrier,
                inc=1,
                device_id={axis: lax.rem(place + turn, count)},
                device_id_type=MESH,
            )
    for has_neighbour, neighbour in ((gz > 0, gz - 1), (gz < nz - 1, gz + 1)):
        @pl.when(has_neighbour)
        def _():
            pl.semaphore_signal(
                barrier, inc=1, device_id={"gz": neighbour}, device_id_type=MESH
            )

    at_end = (gz == 0) | (gz == nz - 1)

    def load(start, rows, group):
        rows = pl.ds(start, rows)
        return pltpu.make_async_copy(passages.at[rows], x.at[rows], load_sem.at[group])

    group_rows = (per_chunk, block_rows - per_chunk) + (block_rows,) * (half_blocks - 1)
    for group, rows in enumerate(group_rows):
        c = group if group < 2 else (group - 1) * per_block
        load(low_start(c), rows, group).start()
        load(high_start(c), rows, group).start()

    def wait_load(group):
        load(0, 2 * group_rows[group], group).wait()

    for copy in small[1:]:
        copy.wait()

    first_token = (gz * token_count).astype(jnp.float32)
    for b in range(passage_count // 128):
        row = lengths[b : b + 1, :].astype(jnp.float32) - first_token
        limits[b * 128 : (b + 1) * 128, :] = jnp.broadcast_to(row, (128, 128)).T

    small[0].wait()
    wide_queries[...] = queries[...].astype(jnp.float32).reshape(row_count, width)
    for i in range(query_rows):
        tile = wide_queries[pl.ds(i, query_count, stride=query_rows), :]
        query_columns[:, i * query_count : (i + 1) * query_count] = tile.T.astype(jnp.bfloat16)

    token_ids = lax.broadcasted_iota(jnp.int32, (token_count, width), 0).astype(jnp.float32)
    tile_columns = 256

    def compute(*halves):
        rows = len(halves) * per_chunk
        limit = []
        for place, (side, c) in enumerate(halves):
            start = jnp.where(side == 0, low_start(c), high_start(c))
            for p in range(per_chunk):
                tokens = x[start + p].astype(jnp.float32)
                usable = token_ids < limits[pl.ds(start + p, 1), :]
                tokens = jnp.where(usable, tokens, tokens[0:1, :])
                row = (place * per_chunk + p) * token_count
                masked_x[row : row + token_count, :] = tokens.astype(jnp.bfloat16)
            limit.append(limits[pl.ds(start, per_chunk), :])
        limit = jnp.concatenate(limit, axis=0)
        any_used = jnp.concatenate([limit] * (tile_columns // 128), axis=1) > 0.0
        for t in range(row_count // tile_columns):
            columns = slice(t * tile_columns, (t + 1) * tile_columns)
            scores = jnp.dot(
                masked_x[0 : rows * token_count, :],
                query_columns[:, columns],
                preferred_element_type=jnp.float32,
            )
            best = jnp.max(scores.reshape(rows, token_count, tile_columns), axis=1)
            best = jnp.where(any_used, best, masked_low)
            for place, (side, c) in enumerate(halves):
                own[side, c, :, columns] = best[place * per_chunk : (place + 1) * per_chunk]

    class Flow:
        def __init__(self, side, hops, lags, target):
            self.side, self.target = side, target
            self.is_first, self.is_last = hops == 0, hops == nz - 1
            self.is_inner = (hops > 0) & (hops < nz - 1)
            even, odd = (start + more * (hops - 1) for start, more in lags)
            self.lag = jnp.where(lax.rem(gx, 2) == 0, even, odd)

        def copy(self, source, where, index):
            return pltpu.make_async_remote_copy(
                src_ref=source.at[(self.side, *where)],
                dst_ref=got.at[(self.side, *where)],
                send_sem=z_send.at[self.side],
                recv_sem=z_recv.at[self.side, index],
                device_id={"gz": self.target},
                device_id_type=MESH,
            )

        def merge(self, where):
            where = (self.side, *where)
            got[where] = jnp.maximum(got[where], own[where])

    def pieces(c, act):
        @pl.when(c < chunks - 1)
        def _():
            act((c,), c)

        @pl.when(c == chunks - 1)
        def _():
            for part in range(TAIL_PARTS):
                act((c, pl.ds(part * tail_rows, tail_rows)), c + part)

    first, last = gz == 0, gz == nz - 1
    below, above = lax.rem(gz + nz - 1, nz), lax.rem(gz + 1, nz)
    low = Flow(0, nz - 1 - gz, DOWN_LAGS, below)
    high = Flow(1, gz, UP_LAGS, above)
    flows = (low, high)

    def peer_copy(turn, slot, block, where):
        return pltpu.make_async_remote_copy(
            src_ref=partials.at[(slot, *where)],
            dst_ref=partials.at[(slot, *where)],
            send_sem=peer_send,
            recv_sem=peer_recv.at[block],
            device_id={"gy": lax.rem(gy + turn, ny)},
            device_id_type=MESH,
        )

    def finalise(side, c):
        counted = query_len[...] - gy * query_rows
        so_far = jnp.zeros((per_chunk, query_count), jnp.float32)
        for i in range(query_rows):
            values = got[side, c, :, i * query_count : (i + 1) * query_count]
            so_far = so_far + jnp.where(counted > i, values, 0.0)
        partials[gy, c] = so_far

        @pl.when(last & (c >= chunks - TAIL))
        def _():
            for turn in reversed(range(ny)):
                far_copy(turn, gy, c - (chunks - TAIL)).start()

        for turn in range(1, ny):
            peer_copy(turn, gy, piece_of(c), (c,)).start()

    def wait_landed(whole, sem):
        pltpu.make_async_remote_copy(
            src_ref=whole,
            dst_ref=whole,
            send_sem=peer_send,
            recv_sem=sem,
            device_id={"gz": below},
            device_id_type=MESH,
        ).wait_recv()

    def piece_of(c):
        return c // per_block + jnp.where(c >= chunks - TAIL, 1, 0)

    def piece_total(piece):
        start = piece * per_block if piece < half_blocks else chunks - TAIL
        count = TAIL if piece == half_blocks else per_block - TAIL * (piece == half_blocks - 1)
        where = pl.ds(start, count)
        wait_landed(partials.at[pl.ds(0, ny - 1), where], peer_recv.at[piece])
        summed = partials[0, where]
        for slot in range(1, ny):
            summed = summed + partials[slot, where]
        return summed.reshape(count * per_chunk, query_count)

    def far_copy(turn, slot, piece):
        return pltpu.make_async_remote_copy(
            src_ref=partials.at[slot, chunks - TAIL + piece],
            dst_ref=far_tail.at[slot, piece],
            send_sem=far_send,
            recv_sem=far_recv,
            device_id={"gy": lax.rem(gy + turn, ny), "gz": 0},
            device_id_type=MESH,
        )

    def forward_copy(block):
        target = jnp.where(gz == 0, half_blocks - 1 - block, half_blocks + block)
        return pltpu.make_async_remote_copy(
            src_ref=forward.at[block],
            dst_ref=total,
            send_sem=forward_send.at[block],
            recv_sem=forward_recv,
            device_id={"gz": target},
            device_id_type=MESH,
        )

    urgent = jnp.where(gz < half_blocks, 1, 0)

    def pass_on(s):
        for flow in flows:
            c = s - flow.lag

            @pl.when(flow.is_inner & (c >= 0) & (c < chunks))
            def _():
                def act(where, index):
                    flow.copy(got, where, index).wait_recv()
                    flow.merge(where)
                    flow.copy(got, where, index).start()

                pieces(c, act)

    def send(c):
        for flow in flows:
            @pl.when(flow.is_first)
            def _():
                pieces(c, lambda where, index: flow.copy(own, where, index).start())

    def step(s, carry):
        pass_on(s)
        for group in range(1, len(group_rows)):
            @pl.when(s == (1 if group == 1 else (group - 1) * per_block))
            def _():
                wait_load(group)

        compute((urgent, s), (1 - urgent, s - 1))
        send(s)
        return carry

    def drain(s, carry):
        pass_on(s)
        return carry

    wait_load(0)
    compute((urgent, 0))
    pl.semaphore_wait(barrier, nx + ny - 2 + jnp.where(at_end, 1, 2))
    send(0)
    lax.fori_loop(1, chunks, step, 0)
    pass_on(chunks)
    compute((1 - urgent, chunks - 1))

    @pl.when(jnp.logical_not(at_end))
    def _():
        last_lag = max(start + more * (nz - 3) for start, more in UP_LAGS + DOWN_LAGS)
        lax.fori_loop(chunks + 1, chunks + last_lag, drain, 0)

    for flow in flows:
        @pl.when(flow.is_last)
        def _():
            def collect(c, carry):
                def act(where, index):
                    flow.copy(got, where, index).wait_recv()
                    flow.merge(where)

                pieces(c, act)
                finalise(flow.side, c)
                for block in range(half_blocks - 1):
                    @pl.when(c == (block + 1) * per_block - 1 + PEER_LAG)
                    def _():
                        forward[block] = piece_total(block)
                        forward_copy(block).start()
                return carry

            lax.fori_loop(0, chunks, collect, 0)

    main_rows = block_rows - TAIL * per_chunk
    row_ids = lax.broadcasted_iota(jnp.int32, stats.shape[1:], 0)

    def stat_copy(slot, to_x, to_y, to_z, kind=0):
        return pltpu.make_async_remote_copy(
            src_ref=stats.at[slot],
            dst_ref=stats.at[slot],
            send_sem=stat_send,
            recv_sem=stat_recv.at[kind],
            device_id={"gx": to_x, "gy": to_y, "gz": to_z},
            device_id_type=MESH,
        )

    def pair(top, summed):
        return jnp.where(row_ids == 0, top, summed)

    def joined(pairs):
        highest = functools.reduce(jnp.maximum, [top for top, _ in pairs])
        shares = [summed * jnp.exp(top - highest) for top, summed in pairs]
        return highest, functools.reduce(jnp.add, shares)

    def summary(blocks):
        tops = [jnp.max(block, axis=0, keepdims=True) for block in blocks]
        top = functools.reduce(jnp.maximum, tops)
        sums = [jnp.sum(jnp.exp(block - top), axis=0, keepdims=True) for block in blocks]
        return top, functools.reduce(jnp.add, sums)

    def read(slot):
        return stats[slot, 0:1, :], stats[slot, 1:2, :]

    def main_summary():
        total[pl.ds(0, main_rows), :] = piece_total(half_blocks - 1)
        blocks = [forward[block] for block in range(half_blocks - 1)]
        return summary(blocks + [total[pl.ds(0, main_rows), :]])

    far_stat = stat_copy(nx, gx, gy, 0, 1)
    beside = [lax.rem(gx + turn, nx) for turn in range(1, nx)]
    column = [
        (lax.rem(gx + turn, nx), to_z)
        for to_z in reversed(range(1, nz))
        for turn in reversed(range(nx))
    ]
    helper = min(1, ny - 1)
    shared = (nx - 1, nx - 1 + len(column), nx - 1 + 2 * len(column))

    def shares(act):
        @pl.when((gy == 0) & (helper != 0))
        def _():
            act(0)

        @pl.when((gy != helper) & (gy != 0))
        def _():
            act(1)

        @pl.when(gy == helper)
        def _():
            act(2 if helper else 1)


    @pl.when(last)
    def _():
        stats[nx] = pair(*main_summary())
        far_stat.start()
        total[pl.ds(main_rows, TAIL * per_chunk), :] = piece_total(half_blocks)

    @pl.when(jnp.logical_not(at_end))
    def _():
        forward_copy(0).wait_recv()

    @pl.when(first)
    def _():
        main = main_summary()
        total[pl.ds(main_rows, TAIL * per_chunk), :] = piece_total(half_blocks)
        wait_landed(far_tail, far_recv)
        far = functools.reduce(jnp.add, [far_tail[slot] for slot in range(ny)])
        blocks = [total[pl.ds(main_rows, TAIL * per_chunk), :], far.reshape(-1, query_count)]
        far_stat.wait_recv()
        stats[gx] = pair(*joined([main, summary(blocks), read(nx)]))
        for to_x in beside:
            stat_copy(gx, to_x, gy, gz).start()

        def share(columns):
            for to_y in (0, gy)[2 - columns :] if columns else ():
                for to_x, to_z in column:
                    stat_copy(gx, to_x, to_y, to_z).start()

        shares(share)
        wait_landed(stats.at[pl.ds(0, nx - 1)], stat_recv.at[0])

    @pl.when(jnp.logical_not(first))
    def _():
        wait_landed(stats.at[pl.ds(0, nx)], stat_recv.at[0])

    top, summed = joined([read(slot) for slot in range(nx)])
    scores = total[...]
    out[...] = (scores - (top + jnp.log(summed))).T

    def wait_sent(whole, sem):
        pltpu.make_async_remote_copy(
            src_ref=whole,
            dst_ref=whole,
            send_sem=sem,
            recv_sem=forward_recv,
            device_id={"gz": below},
            device_id_type=MESH,
        ).wait_send()

    for flow in flows:
        @pl.when(jnp.logical_not(flow.is_last))
        def _():
            wait_sent(got.at[flow.side], z_send.at[flow.side])

    @pl.when(at_end)
    def _():
        wait_sent(partials.at[pl.ds(0, ny - 1)], peer_send)
        for block in range(half_blocks - 1):
            forward_copy(block).wait_send()

    @pl.when(last)
    def _():
        wait_sent(far_tail, far_send)
        far_stat.wait_send()

    @pl.when(first)
    def _():
        shares(lambda columns: wait_sent(stats.at[pl.ds(0, shared[columns])], stat_send))


def shards(sizes, queries, passages, passage_len, query_len):
    nx, ny, nz = sizes
    query_count, query_rows, width = queries.shape
    passage_count, token_count, _ = passages.shape
    row_count = query_count * query_rows
    block_rows = passage_count // nz
    per_chunk = PER_CHUNK
    chunks = passage_count // 2 // per_chunk
    half_blocks = nz // 2
    maxima = pltpu.VMEM((2, chunks, per_chunk, row_count), jnp.float32)
    dma = pltpu.SemaphoreType.DMA
    anywhere = pl.BlockSpec(memory_space=pltpu.HBM)
    return pl.pallas_call(
        functools.partial(kernel, sizes),
        out_shape=pltpu.VMEM((query_count, block_rows), jnp.float32),
        in_specs=[anywhere] * 4,
        out_specs=pl.BlockSpec(memory_space=pltpu.VMEM),
        scratch_shapes=[
            pltpu.VMEM(queries.shape, queries.dtype),
            pltpu.VMEM((passage_count // 128, 128), passage_len.dtype),
            pltpu.VMEM((1, query_count), query_len.dtype),
            pltpu.VMEM(passages.shape, passages.dtype),
            pltpu.VMEM((2 * per_chunk * token_count, width), jnp.bfloat16),
            pltpu.VMEM((row_count, width), jnp.float32),
            pltpu.VMEM((width, row_count), jnp.bfloat16),
            pltpu.VMEM((passage_count, 128), jnp.float32),
            maxima,
            maxima,
            pltpu.VMEM((ny, chunks, per_chunk, query_count), jnp.float32),
            pltpu.VMEM((max(1, half_blocks - 1), block_rows, query_count), jnp.float32),
            pltpu.VMEM((block_rows, query_count), jnp.float32),
            pltpu.VMEM((nx * (2 * nz - 1), 8, query_count), jnp.float32),
            pltpu.VMEM((ny, TAIL, per_chunk, query_count), jnp.float32),
            dma((3,)),
            dma((half_blocks + 1,)),
            dma((2,)),
            dma((2, chunks + TAIL_PARTS - 1)),
            dma,
            dma((half_blocks + 1,)),
            dma((max(1, half_blocks - 1),)),
            dma,
            dma,
            dma((2,)),
            dma,
            dma,
        ],
        compiler_params=pltpu.CompilerParams(
            collective_id=0, has_side_effects=True, vmem_limit_bytes=VMEM_BYTES - 4 * query_count * block_rows
        ),
    )(
        queries,
        passage_len.reshape(passage_count // 128, 128),
        query_len.reshape(1, query_count),
        passages,
    )


def solution(mesh):
    sizes = tuple(mesh.shape[name] for name in ("gx", "gy", "gz"))
    return jax.shard_map(
        functools.partial(shards, sizes),
        mesh=mesh,
        in_specs=(P(None, "gy", None), P("gx", "gz", None), P("gx"), P()),
        out_specs=P(None, ("gx", "gz")),
        check_vma=False,
    )
```

```python
import functools

import jax
import jax.numpy as jnp
from jax import lax
from jax.experimental import pallas as pl
from jax.experimental.pallas import tpu as pltpu
from jax.sharding import PartitionSpec as P

masked_low = -1e30
MESH = pl.DeviceIdType.MESH
UP_LAGS = ((3, 3), (2, 2))
DOWN_LAGS = ((4, 3), (2, 2))
TAIL_PARTS = 2
PEER_LAG = 3
TAIL = 2
VMEM_BYTES = 67043328
PER_CHUNK = 16


def kernel(
    sizes,
    queries_in,
    lengths_in,
    query_len_in,
    passages,
    out,
    queries,
    lengths,
    query_len,
    x,
    masked_x,
    wide_queries,
    query_columns,
    limits,
    own,
    got,
    partials,
    forward,
    total,
    stats,
    far_tail,
    small_sem,
    load_sem,
    z_send,
    z_recv,
    peer_send,
    peer_recv,
    forward_send,
    forward_recv,
    stat_send,
    stat_recv,
    far_send,
    far_recv,
):
    nx, ny, nz = sizes
    gx, gy, gz = (lax.axis_index(name) for name in ("gx", "gy", "gz"))
    passage_count, token_count, width = x.shape
    query_count, query_rows, _ = queries.shape
    _, chunks, per_chunk, row_count = own.shape
    tail_rows = per_chunk // TAIL_PARTS
    half_blocks = nz // 2
    per_block = chunks // half_blocks
    block_rows = passage_count // nz

    def low_start(c):
        return (half_blocks - 1 - c // per_block) * block_rows + (c % per_block) * per_chunk

    def high_start(c):
        return half_blocks * block_rows + c * per_chunk

    small = [
        pltpu.make_async_copy(source, target, small_sem.at[index])
        for index, (source, target) in enumerate(
            ((queries_in, queries), (lengths_in, lengths), (query_len_in, query_len))
        )
    ]
    for copy in small:
        copy.start()

    barrier = pltpu.get_barrier_semaphore()
    for axis, place, count in (("gx", gx, nx), ("gy", gy, ny)):
        for turn in range(1, count):
            pl.semaphore_signal(
                barrier,
                inc=1,
                device_id={axis: lax.rem(place + turn, count)},
                device_id_type=MESH,
            )
    for has_neighbour, neighbour in ((gz > 0, gz - 1), (gz < nz - 1, gz + 1)):
        @pl.when(has_neighbour)
        def _():
            pl.semaphore_signal(
                barrier, inc=1, device_id={"gz": neighbour}, device_id_type=MESH
            )

    at_end = (gz == 0) | (gz == nz - 1)

    def load(start, rows, group):
        rows = pl.ds(start, rows)
        return pltpu.make_async_copy(passages.at[rows], x.at[rows], load_sem.at[group])

    group_rows = (per_chunk, block_rows - per_chunk) + (block_rows,) * (half_blocks - 1)
    for group, rows in enumerate(group_rows):
        c = group if group < 2 else (group - 1) * per_block
        load(low_start(c), rows, group).start()
        load(high_start(c), rows, group).start()

    def wait_load(group):
        load(0, 2 * group_rows[group], group).wait()

    for copy in small[1:]:
        copy.wait()

    first_token = (gz * token_count).astype(jnp.float32)
    for b in range(passage_count // 128):
        row = lengths[b : b + 1, :].astype(jnp.float32) - first_token
        limits[b * 128 : (b + 1) * 128, :] = jnp.broadcast_to(row, (128, 128)).T

    small[0].wait()
    wide_queries[...] = queries[...].astype(jnp.float32).reshape(row_count, width)
    for i in range(query_rows):
        tile = wide_queries[pl.ds(i, query_count, stride=query_rows), :]
        query_columns[:, i * query_count : (i + 1) * query_count] = tile.T.astype(jnp.bfloat16)

    token_ids = lax.broadcasted_iota(jnp.int32, (token_count, width), 0).astype(jnp.float32)
    tile_columns = 256

    def compute(*halves):
        rows = len(halves) * per_chunk
        limit = []
        for place, (side, c) in enumerate(halves):
            start = jnp.where(side == 0, low_start(c), high_start(c))
            for p in range(per_chunk):
                tokens = x[start + p].astype(jnp.float32)
                usable = token_ids < limits[pl.ds(start + p, 1), :]
                tokens = jnp.where(usable, tokens, tokens[0:1, :])
                row = (place * per_chunk + p) * token_count
                masked_x[row : row + token_count, :] = tokens.astype(jnp.bfloat16)
            limit.append(limits[pl.ds(start, per_chunk), :])
        limit = jnp.concatenate(limit, axis=0)
        any_used = jnp.concatenate([limit] * (tile_columns // 128), axis=1) > 0.0
        for t in range(row_count // tile_columns):
            columns = slice(t * tile_columns, (t + 1) * tile_columns)
            scores = jnp.dot(
                masked_x[0 : rows * token_count, :],
                query_columns[:, columns],
                preferred_element_type=jnp.float32,
            )
            best = jnp.max(scores.reshape(rows, token_count, tile_columns), axis=1)
            best = jnp.where(any_used, best, masked_low)
            for place, (side, c) in enumerate(halves):
                own[side, c, :, columns] = best[place * per_chunk : (place + 1) * per_chunk]

    class Flow:
        def __init__(self, side, hops, lags, target):
            self.side, self.target = side, target
            self.is_first, self.is_last = hops == 0, hops == nz - 1
            self.is_inner = (hops > 0) & (hops < nz - 1)
            even, odd = (start + more * (hops - 1) for start, more in lags)
            self.lag = jnp.where(lax.rem(gx, 2) == 0, even, odd)

        def copy(self, source, where, index):
            return pltpu.make_async_remote_copy(
                src_ref=source.at[(self.side, *where)],
                dst_ref=got.at[(self.side, *where)],
                send_sem=z_send.at[self.side],
                recv_sem=z_recv.at[self.side, index],
                device_id={"gz": self.target},
                device_id_type=MESH,
            )

        def merge(self, where):
            where = (self.side, *where)
            got[where] = jnp.maximum(got[where], own[where])

    def pieces(c, act):
        @pl.when(c < chunks - 1)
        def _():
            act((c,), c)

        @pl.when(c == chunks - 1)
        def _():
            for part in range(TAIL_PARTS):
                act((c, pl.ds(part * tail_rows, tail_rows)), c + part)

    first, last = gz == 0, gz == nz - 1
    below, above = lax.rem(gz + nz - 1, nz), lax.rem(gz + 1, nz)
    low = Flow(0, nz - 1 - gz, DOWN_LAGS, below)
    high = Flow(1, gz, UP_LAGS, above)
    flows = (low, high)

    def peer_copy(turn, slot, block, where):
        return pltpu.make_async_remote_copy(
            src_ref=partials.at[(slot, *where)],
            dst_ref=partials.at[(slot, *where)],
            send_sem=peer_send,
            recv_sem=peer_recv.at[block],
            device_id={"gy": lax.rem(gy + turn, ny)},
            device_id_type=MESH,
        )

    def finalise(side, c):
        counted = query_len[...] - gy * query_rows
        so_far = jnp.zeros((per_chunk, query_count), jnp.float32)
        for i in range(query_rows):
            values = got[side, c, :, i * query_count : (i + 1) * query_count]
            so_far = so_far + jnp.where(counted > i, values, 0.0)
        partials[gy, c] = so_far

        @pl.when(last & (c >= chunks - TAIL))
        def _():
            for turn in reversed(range(ny)):
                far_copy(turn, gy, c - (chunks - TAIL)).start()

        for turn in reversed(range(1, ny)):
            peer_copy(turn, gy, piece_of(c), (c,)).start()

    def wait_landed(whole, sem):
        pltpu.make_async_remote_copy(
            src_ref=whole,
            dst_ref=whole,
            send_sem=peer_send,
            recv_sem=sem,
            device_id={"gz": below},
            device_id_type=MESH,
        ).wait_recv()

    def piece_of(c):
        return c // per_block + jnp.where(c >= chunks - TAIL, 1, 0)

    def piece_total(piece):
        start = piece * per_block if piece < half_blocks else chunks - TAIL
        count = TAIL if piece == half_blocks else per_block - TAIL * (piece == half_blocks - 1)
        where = pl.ds(start, count)
        wait_landed(partials.at[pl.ds(0, ny - 1), where], peer_recv.at[piece])
        summed = partials[0, where]
        for slot in range(1, ny):
            summed = summed + partials[slot, where]
        return summed.reshape(count * per_chunk, query_count)

    def far_copy(turn, slot, piece):
        return pltpu.make_async_remote_copy(
            src_ref=partials.at[slot, chunks - TAIL + piece],
            dst_ref=far_tail.at[slot, piece],
            send_sem=far_send,
            recv_sem=far_recv,
            device_id={"gy": lax.rem(gy + turn, ny), "gz": 0},
            device_id_type=MESH,
        )

    def forward_copy(block):
        target = jnp.where(gz == 0, half_blocks - 1 - block, half_blocks + block)
        return pltpu.make_async_remote_copy(
            src_ref=forward.at[block],
            dst_ref=total,
            send_sem=forward_send.at[block],
            recv_sem=forward_recv,
            device_id={"gz": target},
            device_id_type=MESH,
        )

    urgent = jnp.where(gz < half_blocks, 1, 0)

    def pass_on(s):
        for flow in flows:
            c = s - flow.lag

            @pl.when(flow.is_inner & (c >= 0) & (c < chunks))
            def _():
                def act(where, index):
                    flow.copy(got, where, index).wait_recv()
                    flow.merge(where)
                    flow.copy(got, where, index).start()

                pieces(c, act)

    def send(c):
        for flow in flows:
            @pl.when(flow.is_first)
            def _():
                pieces(c, lambda where, index: flow.copy(own, where, index).start())

    def step(s, carry):
        pass_on(s)
        for group in range(1, len(group_rows)):
            @pl.when(s == (1 if group == 1 else (group - 1) * per_block))
            def _():
                wait_load(group)

        compute((urgent, s), (1 - urgent, s - 1))
        send(s)
        return carry

    def drain(s, carry):
        pass_on(s)
        return carry

    wait_load(0)
    compute((urgent, 0))
    pl.semaphore_wait(barrier, nx + ny - 2 + jnp.where(at_end, 1, 2))
    send(0)
    lax.fori_loop(1, chunks, step, 0)
    pass_on(chunks)
    compute((1 - urgent, chunks - 1))

    @pl.when(jnp.logical_not(at_end))
    def _():
        last_lag = max(start + more * (nz - 3) for start, more in UP_LAGS + DOWN_LAGS)
        lax.fori_loop(chunks + 1, chunks + last_lag, drain, 0)

    for flow in flows:
        @pl.when(flow.is_last)
        def _():
            def collect(c, carry):
                def act(where, index):
                    flow.copy(got, where, index).wait_recv()
                    flow.merge(where)

                pieces(c, act)
                finalise(flow.side, c)
                for block in range(half_blocks - 1):
                    @pl.when(c == (block + 1) * per_block - 1 + PEER_LAG)
                    def _():
                        forward[block] = piece_total(block)
                        forward_copy(block).start()
                return carry

            lax.fori_loop(0, chunks, collect, 0)

    main_rows = block_rows - TAIL * per_chunk
    row_ids = lax.broadcasted_iota(jnp.int32, stats.shape[1:], 0)

    def stat_copy(slot, to_x, to_y, to_z, kind=0):
        return pltpu.make_async_remote_copy(
            src_ref=stats.at[slot],
            dst_ref=stats.at[slot],
            send_sem=stat_send,
            recv_sem=stat_recv.at[kind],
            device_id={"gx": to_x, "gy": to_y, "gz": to_z},
            device_id_type=MESH,
        )

    def pair(top, summed):
        return jnp.where(row_ids == 0, top, summed)

    def joined(pairs):
        highest = functools.reduce(jnp.maximum, [top for top, _ in pairs])
        shares = [summed * jnp.exp(top - highest) for top, summed in pairs]
        return highest, functools.reduce(jnp.add, shares)

    def summary(blocks):
        tops = [jnp.max(block, axis=0, keepdims=True) for block in blocks]
        top = functools.reduce(jnp.maximum, tops)
        sums = [jnp.sum(jnp.exp(block - top), axis=0, keepdims=True) for block in blocks]
        return top, functools.reduce(jnp.add, sums)

    def read(slot):
        return stats[slot, 0:1, :], stats[slot, 1:2, :]

    def main_summary():
        total[pl.ds(0, main_rows), :] = piece_total(half_blocks - 1)
        blocks = [forward[block] for block in range(half_blocks - 1)]
        return summary(blocks + [total[pl.ds(0, main_rows), :]])

    far_stat = stat_copy(nx, gx, gy, 0, 1)
    beside = [lax.rem(gx + turn, nx) for turn in range(1, nx)]
    column = [
        (lax.rem(gx + turn, nx), to_z)
        for to_z in reversed(range(1, nz))
        for turn in reversed(range(nx))
    ]
    helper = min(1, ny - 1)
    shared = (nx - 1, nx - 1 + len(column), nx - 1 + 2 * len(column))

    def shares(act):
        @pl.when((gy == 0) & (helper != 0))
        def _():
            act(0)

        @pl.when((gy != helper) & (gy != 0))
        def _():
            act(1)

        @pl.when(gy == helper)
        def _():
            act(2 if helper else 1)


    @pl.when(last)
    def _():
        stats[nx] = pair(*main_summary())
        far_stat.start()
        total[pl.ds(main_rows, TAIL * per_chunk), :] = piece_total(half_blocks)

    @pl.when(jnp.logical_not(at_end))
    def _():
        forward_copy(0).wait_recv()

    @pl.when(first)
    def _():
        main = main_summary()
        total[pl.ds(main_rows, TAIL * per_chunk), :] = piece_total(half_blocks)
        wait_landed(far_tail, far_recv)
        far = functools.reduce(jnp.add, [far_tail[slot] for slot in range(ny)])
        blocks = [total[pl.ds(main_rows, TAIL * per_chunk), :], far.reshape(-1, query_count)]
        far_stat.wait_recv()
        stats[gx] = pair(*joined([main, summary(blocks), read(nx)]))
        for to_x in beside:
            stat_copy(gx, to_x, gy, gz).start()

        def share(columns):
            for to_y in (0, gy)[2 - columns :] if columns else ():
                for to_x, to_z in column:
                    stat_copy(gx, to_x, to_y, to_z).start()

        shares(share)
        wait_landed(stats.at[pl.ds(0, nx - 1)], stat_recv.at[0])

    @pl.when(jnp.logical_not(first))
    def _():
        wait_landed(stats.at[pl.ds(0, nx)], stat_recv.at[0])

    top, summed = joined([read(slot) for slot in range(nx)])
    scores = total[...]
    out[...] = (scores - (top + jnp.log(summed))).T

    def wait_sent(whole, sem):
        pltpu.make_async_remote_copy(
            src_ref=whole,
            dst_ref=whole,
            send_sem=sem,
            recv_sem=forward_recv,
            device_id={"gz": below},
            device_id_type=MESH,
        ).wait_send()

    for flow in flows:
        @pl.when(jnp.logical_not(flow.is_last))
        def _():
            wait_sent(got.at[flow.side], z_send.at[flow.side])

    @pl.when(at_end)
    def _():
        wait_sent(partials.at[pl.ds(0, ny - 1)], peer_send)
        for block in range(half_blocks - 1):
            forward_copy(block).wait_send()

    @pl.when(last)
    def _():
        wait_sent(far_tail, far_send)
        far_stat.wait_send()

    @pl.when(first)
    def _():
        shares(lambda columns: wait_sent(stats.at[pl.ds(0, shared[columns])], stat_send))


def shards(sizes, queries, passages, passage_len, query_len):
    nx, ny, nz = sizes
    query_count, query_rows, width = queries.shape
    passage_count, token_count, _ = passages.shape
    row_count = query_count * query_rows
    block_rows = passage_count // nz
    per_chunk = PER_CHUNK
    chunks = passage_count // 2 // per_chunk
    half_blocks = nz // 2
    maxima = pltpu.VMEM((2, chunks, per_chunk, row_count), jnp.float32)
    dma = pltpu.SemaphoreType.DMA
    anywhere = pl.BlockSpec(memory_space=pltpu.HBM)
    return pl.pallas_call(
        functools.partial(kernel, sizes),
        out_shape=pltpu.VMEM((query_count, block_rows), jnp.float32),
        in_specs=[anywhere] * 4,
        out_specs=pl.BlockSpec(memory_space=pltpu.VMEM),
        scratch_shapes=[
            pltpu.VMEM(queries.shape, queries.dtype),
            pltpu.VMEM((passage_count // 128, 128), passage_len.dtype),
            pltpu.VMEM((1, query_count), query_len.dtype),
            pltpu.VMEM(passages.shape, passages.dtype),
            pltpu.VMEM((2 * per_chunk * token_count, width), jnp.bfloat16),
            pltpu.VMEM((row_count, width), jnp.float32),
            pltpu.VMEM((width, row_count), jnp.bfloat16),
            pltpu.VMEM((passage_count, 128), jnp.float32),
            maxima,
            maxima,
            pltpu.VMEM((ny, chunks, per_chunk, query_count), jnp.float32),
            pltpu.VMEM((max(1, half_blocks - 1), block_rows, query_count), jnp.float32),
            pltpu.VMEM((block_rows, query_count), jnp.float32),
            pltpu.VMEM((nx * (2 * nz - 1), 8, query_count), jnp.float32),
            pltpu.VMEM((ny, TAIL, per_chunk, query_count), jnp.float32),
            dma((3,)),
            dma((half_blocks + 1,)),
            dma((2,)),
            dma((2, chunks + TAIL_PARTS - 1)),
            dma,
            dma((half_blocks + 1,)),
            dma((max(1, half_blocks - 1),)),
            dma,
            dma,
            dma((2,)),
            dma,
            dma,
        ],
        compiler_params=pltpu.CompilerParams(
            collective_id=0, has_side_effects=True, vmem_limit_bytes=VMEM_BYTES - 4 * query_count * block_rows
        ),
    )(
        queries,
        passage_len.reshape(passage_count // 128, 128),
        query_len.reshape(1, query_count),
        passages,
    )


def solution(mesh):
    sizes = tuple(mesh.shape[name] for name in ("gx", "gy", "gz"))
    return jax.shard_map(
        functools.partial(shards, sizes),
        mesh=mesh,
        in_specs=(P(None, "gy", None), P("gx", "gz", None), P("gx"), P()),
        out_specs=P(None, ("gx", "gz")),
        check_vma=False,
    )
```
